8 devices in a mesh: dp: 2 (over z, y), tp: 4 (over x, core).
Axes of the slice: x: 2, y: 2, z: 1, core: 2. Of those that a mesh axis runs over, the one named last changes fastest.
Arguments:
- hidden: bfloat16 [32, 896], P('dp'), parts along dimension 0
- final_gain: bfloat16 [896], replicated
- embed_table: bfloat16 [151936, 896], P(None, 'tp')
- targets: int32 [32], P('dp'), parts along dimension 0
- temperature: float32 [], replicated
Outputs:
- output 1: float32 [32], P('dp'), parts along dimension 0
- output 2: float32 [32], P('dp'), parts along dimension 0
- output 3: bfloat16 [32, 151936], P('dp', 'tp'), parts along dimension 0
There are 2 independent parts. The reference program is written for one: setup_inputs(seed, part) draws one part's arguments, and reference() takes and returns one part's arrays. A program takes and returns all parts, laid end to end along the dimension named above; an argument that names none is the same for every part.
All inputs are finite; a program needn't handle non-finite values.
Results may differ from the reference program's by a relative error of at most 0.0011657.
Values sent between devices are 32-bit elements.
A program may use at most 1 GiB of HBM per device.

```python
import jax
import jax.numpy as jnp
from jax import lax

TOKENS = 16
HIDDEN = 896
VOCABULARY = 151936
NORM_EPS = 1e-6
ROW_BLOCK = min(TOKENS, 32)


def setup_inputs(seed: int = 0, part: int = 0) -> dict:
    shared_key, part_root = jax.random.split(jax.random.key(seed))
    part_key = jax.random.fold_in(part_root, part)
    gain_key, table_key, temp_key = jax.random.split(shared_key, 3)
    hidden_key, perm_key, offset_key = jax.random.split(part_key, 3)
    hidden = jax.random.normal(hidden_key, (TOKENS, HIDDEN), jnp.float32).astype(jnp.bfloat16)
    final_gain = jax.random.uniform(gain_key, (HIDDEN,), jnp.float32, 0.5, 1.5).astype(jnp.bfloat16)
    embed_table = (jax.random.normal(table_key, (VOCABULARY, HIDDEN), jnp.float32) * (2.0 / HIDDEN ** 0.5)).astype(jnp.bfloat16)
    stride = VOCABULARY // TOKENS
    targets = (jax.random.permutation(perm_key, TOKENS).astype(jnp.int32) * stride
               + jax.random.randint(offset_key, (TOKENS,), 0, stride, jnp.int32))
    temperature = jax.random.uniform(temp_key, (), jnp.float32, 0.8, 1.25)
    return {'hidden': hidden, 'final_gain': final_gain, 'embed_table': embed_table,
            'targets': targets, 'temperature': temperature}


def reference(hidden, final_gain, embed_table, targets, temperature):
    hidden_f32 = hidden.astype(jnp.float32)
    inv_rms = lax.rsqrt(jnp.mean(hidden_f32 * hidden_f32, axis=-1, keepdims=True) + NORM_EPS)
    normed = (hidden_f32 * inv_rms * final_gain.astype(jnp.float32)).astype(jnp.bfloat16)
    num_blocks = TOKENS // ROW_BLOCK
    normed_blocks = normed.reshape(num_blocks, ROW_BLOCK, HIDDEN)
    target_blocks = targets.reshape(num_blocks, ROW_BLOCK)

    def score_block(block_pair):
        normed_rows, target_ids = block_pair
        logits = jnp.dot(normed_rows, embed_table.T, preferred_element_type=jnp.float32) / temperature
        row_max = jnp.max(logits, axis=-1, keepdims=True)
        log_norm = row_max[:, 0] + jnp.log(jnp.sum(jnp.exp(logits - row_max), axis=-1))
        target_logit = jnp.take_along_axis(logits, target_ids[:, None], axis=1)[:, 0]
        token_probs = jnp.exp(logits - log_norm[:, None]).astype(jnp.bfloat16)
        return log_norm, target_logit - log_norm, token_probs

    log_norm, target_logprob, token_probs = lax.map(score_block, (normed_blocks, target_blocks))
    return (log_norm.reshape(TOKENS), target_logprob.reshape(TOKENS),
            token_probs.reshape(TOKENS, VOCABULARY))
```

```python
import math

import jax
import jax.numpy as jnp
from jax import lax
from jax.experimental import pallas as pl
from jax.experimental.pallas import tpu as pltpu
from jax.sharding import PartitionSpec as P

NORM_EPS = 1e-6
LANES = 128
LOG2E = math.log2(math.e)
LN2 = math.log(2.0)
NBLK = 11
DEPTH = 4
LAG = 3


def head_kernel(rows, vocab, tp,
                hid_ref, gain_ref, tgt_ref, temp_ref, tab_ref,
                probs_ref, ln_ref, tl_ref,
                win, stg, mine, part, rx, mk, stat_out, stat_in, ubuf,
                win_sem, edge_sem, psend, precv, xsend, xrecv, ssend, srecv):
    me = lax.axis_index('tp')
    chip = me // 2
    core = me % 2
    partner = chip * 2 + (1 - core)
    across = (1 - chip) * 2 + core
    diag = (1 - chip) * 2 + (1 - core)
    shard = vocab // tp
    tokens, width = hid_ref.shape
    chunk = NBLK * LANES
    nch = pl.cdiv(shard, chunk)
    steps = 2 * nch
    last_blk = vocab // LANES - 1

    def copies(g, which):
        far = g < nch
        k = jnp.where(far, g, g - nch)
        there = jnp.where(far, 1 - chip, chip)
        dest = there * 2 + (jnp.where(which == 0, 1 - core, core))
        blk = (dest * shard) // LANES + k * NBLK
        slot = (g % DEPTH) * 2 + which
        main = pltpu.make_async_copy(
            tab_ref.at[:, pl.ds(pl.multiple_of(blk * LANES, LANES), chunk)],
            win.at[slot, :, pl.ds(0, chunk)], win_sem.at[slot])
        edge_blk = jnp.minimum(blk + NBLK, last_blk)
        edge = pltpu.make_async_copy(
            tab_ref.at[:, pl.ds(pl.multiple_of(edge_blk * LANES, LANES), LANES)],
            win.at[slot, :, pl.ds(chunk, LANES)], edge_sem.at[slot])
        return main, edge, dest, slot

    def fetch(g):
        for which in range(2):
            main, edge, _, _ = copies(g, which)
            main.start()
            edge.start()

    for g in range(DEPTH):
        fetch(g)

    barrier = pltpu.get_barrier_semaphore()
    for peer in (partner, across, diag):
        pl.semaphore_signal(barrier, inc=1, device_id={'tp': peer},
                            device_id_type=pl.DeviceIdType.MESH)

    x = hid_ref[...].astype(jnp.float32)
    inv_rms = lax.rsqrt(jnp.mean(x * x, axis=-1, keepdims=True) + NORM_EPS)
    u_all = x * inv_rms * gain_ref[...].astype(jnp.float32)
    u = u_all[:, :rows]
    for t in range(1, tp):
        u = jnp.where(me == t, u_all[:, t * rows:(t + 1) * rows], u)
    ubuf[...] = u.astype(jnp.bfloat16)

    lane = lax.broadcasted_iota(jnp.int32, (tokens, LANES), 1)
    row = lax.broadcasted_iota(jnp.int32, (tokens, LANES), 0)

    pl.semaphore_wait(barrier, 3)

    def to_partner(g):
        return pltpu.make_async_remote_copy(
            src_ref=stg.at[g], dst_ref=part.at[g], send_sem=psend.at[g], recv_sem=precv.at[g],
            device_id={'tp': partner}, device_id_type=pl.DeviceIdType.MESH)

    def to_across(k):
        return pltpu.make_async_remote_copy(
            src_ref=mine.at[k], dst_ref=rx.at[k], send_sem=xsend.at[k], recv_sem=xrecv.at[k],
            device_id={'tp': across}, device_id_type=pl.DeviceIdType.MESH)

    def partial_logits(g, which, out):
        main, edge, dest, slot = copies(g, which)
        main.wait()
        edge.wait()
        shift = (dest * shard) % LANES
        back = LANES - shift
        z = jnp.dot(ubuf[...], win[slot], preferred_element_type=jnp.float32)
        rolled = [pltpu.roll(z[:, b * LANES:(b + 1) * LANES], back, 1) for b in range(NBLK + 1)]
        for b in range(NBLK):
            out[g, :, b * LANES:(b + 1) * LANES] = jnp.where(lane < back, rolled[b], rolled[b + 1])

    def combine(g):
        to_partner(g).wait_recv()
        mine[g] = mine[g] + part[g]

    def step(g, _):
        partial_logits(g, 0, stg)
        to_partner(g).start()
        partial_logits(g, 1, mine)

        @pl.when(g + DEPTH < steps)
        def _():
            fetch(g + DEPTH)

        h = g - LAG

        @pl.when(h >= 0)
        def _():
            combine(h)

        @pl.when(jnp.logical_and(h >= 0, h < nch))
        def _():
            to_across(h).start()
        return 0

    lax.fori_loop(0, steps, step, 0)
    for h in range(steps - LAG, steps):
        combine(h)

    factor = LOG2E / temp_ref[0]
    target = jnp.zeros((tokens, LANES), jnp.int32)
    for i in range(tokens):
        target = jnp.where(row == i, tgt_ref[i], target)
    target = target - me * shard

    def absorb(k, carry):
        m, s, tg = carry
        to_across(k).wait_recv()
        ts = []
        new_m = m
        for b in range(NBLK):
            cols = slice(b * LANES, (b + 1) * LANES)
            t = (mine[nch + k, :, cols] + rx[k, :, cols]) * factor
            at = lane + (k * chunk + b * LANES)
            t = jnp.where(at < shard, t, -jnp.inf)
            tg = tg + jnp.where(at == target, t, 0.0)
            new_m = jnp.maximum(new_m, t)
            ts.append(t)
        s = s * jnp.exp2(m - new_m)
        for b in range(NBLK):
            p = jnp.exp2(ts[b] - new_m)
            s = s + p
            mine[nch + k, :, b * LANES:(b + 1) * LANES] = p
        mk[k] = new_m
        return new_m, s, tg

    zeros = jnp.zeros((tokens, LANES), jnp.float32)
    m, s, tg = lax.fori_loop(0, nch, absorb, (zeros - jnp.inf, zeros, zeros))

    top = jnp.max(m, axis=-1, keepdims=True)
    total = jnp.sum(s * jnp.exp2(m - top), axis=-1, keepdims=True)
    tval = jnp.sum(tg, axis=-1, keepdims=True)
    packed = jnp.where(lane == 0, top, jnp.where(lane == 1, total, tval))
    stat_out[...] = packed
    sends = [pltpu.make_async_remote_copy(
        src_ref=stat_out, dst_ref=stat_in.at[i], send_sem=ssend.at[i], recv_sem=srecv.at[i],
        device_id={'tp': peer}, device_id_type=pl.DeviceIdType.MESH)
        for i, peer in enumerate((across, diag, partner))]
    for send in sends:
        send.start()
    for send in sends:
        send.wait_recv()
    others = [stat_in[i] for i in range(3)]
    tops = [top] + [o[:, 0:1] for o in others]
    sums = [total] + [o[:, 1:2] for o in others]
    tvals = [tval] + [o[:, 2:3] for o in others]
    big = tops[0]
    for o in tops[1:]:
        big = jnp.maximum(big, o)
    whole = sum(a * jnp.exp2(o - big) for a, o in zip(sums, tops))
    log2_norm = big + jnp.log2(whole)
    picked = sum(tvals)
    ln_ref[...] = jnp.broadcast_to(log2_norm * LN2, (tokens, LANES))
    tl_ref[...] = jnp.broadcast_to((picked - log2_norm) * LN2, (tokens, LANES))

    for k in range(nch):
        scale = jnp.exp2(mk[k] - log2_norm)
        for b in range(NBLK):
            lo = k * chunk + b * LANES
            hi = min(lo + LANES, shard)
            p = mine[nch + k, :, b * LANES:(b + 1) * LANES] * scale
            probs_ref[:, lo:hi] = p.astype(jnp.bfloat16)[:, :hi - lo]

    for send in sends:
        send.wait_send()

    def drain(g, _):
        to_partner(g).wait_send()

        @pl.when(g < nch)
        def _():
            to_across(g).wait_send()
        return 0

    lax.fori_loop(0, steps, drain, 0)


def solution(mesh):
    tp = mesh.shape['tp']

    def local_scores(hidden, final_gain, table_cols, targets, temperature):
        tokens, width = hidden.shape
        vocab, rows = table_cols.shape
        shard = vocab // tp
        chunk = NBLK * LANES
        nch = pl.cdiv(shard, chunk)
        f32 = jnp.float32

        def body(*refs):
            head_kernel(rows, vocab, tp, *refs)

        vm = pl.BlockSpec(memory_space=pltpu.VMEM)
        sm = pl.BlockSpec(memory_space=pltpu.SMEM)
        probs, ln, tl = pl.pallas_call(
            body,
            out_shape=(jax.ShapeDtypeStruct((tokens, shard), jnp.bfloat16),
                       jax.ShapeDtypeStruct((tokens, LANES), f32),
                       jax.ShapeDtypeStruct((tokens, LANES), f32)),
            in_specs=[vm, vm, sm, sm, pl.BlockSpec(memory_space=pl.ANY)],
            out_specs=(vm, vm, vm),
            scratch_shapes=[
                pltpu.VMEM((DEPTH * 2, rows, chunk + LANES), jnp.bfloat16),
                pltpu.VMEM((2 * nch, tokens, chunk), f32),
                pltpu.VMEM((2 * nch, tokens, chunk), f32),
                pltpu.VMEM((2 * nch, tokens, chunk), f32),
                pltpu.VMEM((nch, tokens, chunk), f32),
                pltpu.VMEM((nch, tokens, LANES), f32),
                pltpu.VMEM((tokens, LANES), f32),
                pltpu.VMEM((3, tokens, LANES), f32),
                pltpu.VMEM((tokens, rows), jnp.bfloat16),
                pltpu.SemaphoreType.DMA((DEPTH * 2,)),
                pltpu.SemaphoreType.DMA((DEPTH * 2,)),
                pltpu.SemaphoreType.DMA((2 * nch,)),
                pltpu.SemaphoreType.DMA((2 * nch,)),
                pltpu.SemaphoreType.DMA((nch,)),
                pltpu.SemaphoreType.DMA((nch,)),
                pltpu.SemaphoreType.DMA((3,)),
                pltpu.SemaphoreType.DMA((3,)),
            ],
            compiler_params=pltpu.CompilerParams(
                collective_id=0, has_side_effects=True,
                vmem_limit_bytes=60 * 1024 * 1024),
        )(hidden, final_gain.reshape(1, width), targets, temperature.reshape(1), table_cols.T)
        return ln[:, 0], tl[:, 0], probs

    return jax.shard_map(local_scores, mesh=mesh,
                         in_specs=(P('dp', None), P(None), P(None, 'tp'), P('dp'), P()),
                         out_specs=(P('dp'), P('dp'), P('dp', 'tp')),
                         check_vma=False)
```

```python
import math

import jax
import jax.numpy as jnp
from jax import lax
from jax.experimental import pallas as pl
from jax.experimental.pallas import tpu as pltpu
from jax.sharding import PartitionSpec as P

NORM_EPS = 1e-6
LANES = 128
LOG2E = math.log2(math.e)
LN2 = math.log(2.0)
NBLK = 11
FINISH_STEPS = 1
DEPTH = 3
LAG = 1


def head_kernel(rows, vocab, tp,
                hid_hbm, gain_hbm, tgt_hbm, temp_ref, tab_ref,
                pexp_ref, peak_ref, stat_ref,
                win, stg, mine, part, rx, stat_out, stat_in, ubuf,
                hid_ref, gain_ref, tgt_ref, in_sem, win_sem, edge_sem, psend, precv, xsend, xrecv, ssend, srecv):
    me = lax.axis_index('tp')
    chip = me // 2
    core = me % 2
    partner = chip * 2 + (1 - core)
    across = (1 - chip) * 2 + core
    diag = (1 - chip) * 2 + (1 - core)
    shard = vocab // tp
    tokens, width = hid_hbm.shape
    chunk = NBLK * LANES
    nch = pl.cdiv(shard, chunk)
    steps = 2 * nch
    last_blk = vocab // LANES - 1

    def copies(g, which):
        far = g < nch
        k = jnp.where(far, g, g - nch)
        there = jnp.where(far, 1 - chip, chip)
        dest = there * 2 + (jnp.where(which == 0, 1 - core, core))
        blk = (dest * shard) // LANES + k * NBLK
        slot = (g % DEPTH) * 2 + which
        main = pltpu.make_async_copy(
            tab_ref.at[:, pl.ds(pl.multiple_of(blk * LANES, LANES), chunk)],
            win.at[slot, :, pl.ds(0, chunk)], win_sem.at[slot])
        edge_blk = jnp.minimum(blk + NBLK, last_blk)
        edge = pltpu.make_async_copy(
            tab_ref.at[:, pl.ds(pl.multiple_of(edge_blk * LANES, LANES), LANES)],
            win.at[slot, :, pl.ds(chunk, LANES)], edge_sem.at[slot])
        return main, edge, dest, slot

    def fetch(g):
        for which in range(2):
            main, edge, _, _ = copies(g, which)
            main.start()
            edge.start()

    barrier = pltpu.get_barrier_semaphore()
    for peer in (partner, across, diag):
        pl.semaphore_signal(barrier, inc=1, device_id={'tp': peer},
                            device_id_type=pl.DeviceIdType.MESH)

    small = [pltpu.make_async_copy(src, dst, in_sem.at[i]) for i, (src, dst) in enumerate((
        (hid_hbm, hid_ref), (gain_hbm, gain_ref), (tgt_hbm, tgt_ref)))]
    for copy in small[:2]:
        copy.start()
    for g in range(DEPTH):
        fetch(g)
    for copy in small[2:]:
        copy.start()
    for copy in small[:2]:
        copy.wait()

    x = hid_ref[...].astype(jnp.float32)
    inv_rms = lax.rsqrt(jnp.mean(x * x, axis=-1, keepdims=True) + NORM_EPS)
    gain = jnp.concatenate([gain_ref[i:i + 1] for i in range(width // LANES)], axis=1).astype(jnp.float32)
    u_all = x * inv_rms * gain
    u = u_all[:, :rows]
    for t in range(1, tp):
        u = jnp.where(me == t, u_all[:, t * rows:(t + 1) * rows], u)
    ubuf[...] = u.astype(jnp.bfloat16)

    lane = lax.broadcasted_iota(jnp.int32, (tokens, LANES), 1)
    row = lax.broadcasted_iota(jnp.int32, (tokens, LANES), 0)

    pl.semaphore_wait(barrier, 3)

    def to_partner(g):
        return pltpu.make_async_remote_copy(
            src_ref=stg.at[g], dst_ref=part.at[g], send_sem=psend.at[g], recv_sem=precv.at[g],
            device_id={'tp': partner}, device_id_type=pl.DeviceIdType.MESH)

    def to_across(k):
        return pltpu.make_async_remote_copy(
            src_ref=mine.at[k], dst_ref=rx.at[k], send_sem=xsend.at[k], recv_sem=xrecv.at[k],
            device_id={'tp': across}, device_id_type=pl.DeviceIdType.MESH)

    def partial_logits(g, which, out):
        main, edge, dest, slot = copies(g, which)
        main.wait()
        edge.wait()
        shift = (dest * shard) % LANES
        back = LANES - shift
        z = jnp.dot(ubuf[...], win[slot], preferred_element_type=jnp.float32)
        rolled = [pltpu.roll(z[:, b * LANES:(b + 1) * LANES], back, 1) for b in range(NBLK + 1)]
        for b in range(NBLK):
            out[g, :, b * LANES:(b + 1) * LANES] = jnp.where(lane < back, rolled[b], rolled[b + 1])

    def combine(g):
        to_partner(g).wait_recv()
        mine[g] = mine[g] + part[g]

    def step(g, _):
        partial_logits(g, 0, stg)
        to_partner(g).start()
        partial_logits(g, 1, mine)

        @pl.when(g + DEPTH < steps)
        def _():
            fetch(g + DEPTH)

        h = g - LAG

        @pl.when(h >= 0)
        def _():
            combine(h)

        @pl.when(jnp.logical_and(h >= 0, h < nch))
        def _():
            to_across(h).start()
        return 0

    lax.fori_loop(0, steps, step, 0)
    for h in range(steps - LAG, steps):
        combine(h)

    for copy in small[2:]:
        copy.wait()
    factor = LOG2E / temp_ref[0]
    target = jnp.zeros((tokens, LANES), jnp.int32)
    for i in range(tokens):
        target = jnp.where(row == i, tgt_ref[i], target)
    target = target - me * shard

    def absorb(k, carry):
        m, s, tg = carry
        to_across(k).wait_recv()
        ts = []
        new_m = m
        for b in range(NBLK):
            cols = slice(b * LANES, (b + 1) * LANES)
            t = (mine[nch + k, :, cols] + rx[k, :, cols]) * factor
            at = lane + (k * chunk + b * LANES)
            t = jnp.where(at < shard, t, -jnp.inf)
            tg = tg + jnp.where(at == target, t, 0.0)
            new_m = jnp.maximum(new_m, t)
            ts.append(t)
        s = s * jnp.exp2(m - new_m)
        for b in range(NBLK):
            p = jnp.exp2(ts[b] - new_m)
            s = s + p
            pexp_ref[k, :, b * LANES:(b + 1) * LANES] = p
        peak_ref[k] = new_m
        return new_m, s, tg

    zeros = jnp.zeros((tokens, LANES), jnp.float32)
    m, s, tg = lax.fori_loop(0, nch, absorb, (zeros - jnp.inf, zeros, zeros))

    top = jnp.max(m, axis=-1, keepdims=True)
    total = jnp.sum(s * jnp.exp2(m - top), axis=-1, keepdims=True)
    tval = jnp.sum(tg, axis=-1, keepdims=True)
    packed = jnp.where(lane == 0, top, jnp.where(lane == 1, total, tval))
    stat_out[...] = packed
    sends = [pltpu.make_async_remote_copy(
        src_ref=stat_out, dst_ref=stat_in.at[i], send_sem=ssend.at[i], recv_sem=srecv.at[i],
        device_id={'tp': peer}, device_id_type=pl.DeviceIdType.MESH)
        for i, peer in enumerate((across, diag, partner))]
    for send in sends:
        send.start()
    for send in sends:
        send.wait_recv()
    others = [stat_in[i] for i in range(3)]
    tops = [top] + [o[:, 0:1] for o in others]
    sums = [total] + [o[:, 1:2] for o in others]
    tvals = [tval] + [o[:, 2:3] for o in others]
    big = tops[0]
    for o in tops[1:]:
        big = jnp.maximum(big, o)
    whole = sum(a * jnp.exp2(o - big) for a, o in zip(sums, tops))
    log2_norm = big + jnp.log2(whole)
    picked = sum(tvals)
    stat_ref[...] = jnp.where(lane == 0, log2_norm, picked)

    for send in sends:
        send.wait_send()

    def drain(g, _):
        to_partner(g).wait_send()

        @pl.when(g < nch)
        def _():
            to_across(g).wait_send()
        return 0

    lax.fori_loop(0, steps, drain, 0)


def finish_kernel(pexp_ref, peak_ref, stat_ref, probs_ref, ln_ref, tl_ref):
    tokens = stat_ref.shape[0]
    log2_norm = stat_ref[:, 0:1]
    picked = stat_ref[:, 1:2]
    group = pexp_ref.shape[0] // FINISH_STEPS
    chunk = pexp_ref.shape[2]
    first = pl.program_id(0) * group
    for i in range(group):
        scale = jnp.exp2(peak_ref[first + i] - log2_norm)
        for b in range(chunk // LANES):
            p = pexp_ref[first + i, :, b * LANES:(b + 1) * LANES] * scale
            probs_ref[:, i * chunk + b * LANES:i * chunk + (b + 1) * LANES] = p.astype(jnp.bfloat16)

    @pl.when(pl.program_id(0) == 0)
    def _():
        lane = lax.broadcasted_iota(jnp.int32, (tokens, LANES), 1)
        row = lax.broadcasted_iota(jnp.int32, (tokens, LANES), 0)
        for out, val in ((ln_ref, log2_norm * LN2), (tl_ref, (picked - log2_norm) * LN2)):
            out[...] = jnp.sum(jnp.where(row == lane, val, 0.0), axis=0)[:tokens]


def solution(mesh):
    tp = mesh.shape['tp']

    def local_scores(hidden, final_gain, table_cols, targets, temperature):
        tokens, width = hidden.shape
        vocab, rows = table_cols.shape
        shard = vocab // tp
        chunk = NBLK * LANES
        nch = pl.cdiv(shard, chunk)
        f32 = jnp.float32

        def body(*refs):
            head_kernel(rows, vocab, tp, *refs)

        vm = pl.BlockSpec(memory_space=pltpu.VMEM)
        def in_hbm(a):
            return pltpu.with_memory_space_constraint(a, pltpu.HBM)

        hbm = pl.BlockSpec(memory_space=pltpu.HBM)
        pexp, peak, stat = pl.pallas_call(
            body,
            out_shape=(pltpu.VMEM((nch, tokens, chunk), f32),
                       pltpu.VMEM((nch, tokens, LANES), f32),
                       pltpu.VMEM((tokens, LANES), f32)),
            in_specs=[hbm, hbm, hbm, pl.BlockSpec(memory_space=pltpu.SMEM), hbm],
            out_specs=(vm, vm, vm),
            scratch_shapes=[
                pltpu.VMEM((DEPTH * 2, rows, chunk + LANES), jnp.bfloat16),
                pltpu.VMEM((2 * nch, tokens, chunk), f32),
                pltpu.VMEM((2 * nch, tokens, chunk), f32),
                pltpu.VMEM((2 * nch, tokens, chunk), f32),
                pltpu.VMEM((nch, tokens, chunk), f32),
                pltpu.VMEM((tokens, LANES), f32),
                pltpu.VMEM((3, tokens, LANES), f32),
                pltpu.VMEM((tokens, rows), jnp.bfloat16),
                pltpu.VMEM((tokens, width), jnp.bfloat16),
                pltpu.VMEM((width // LANES, LANES), jnp.bfloat16),
                pltpu.SMEM((tokens,), jnp.int32),
                pltpu.SemaphoreType.DMA((3,)),
                pltpu.SemaphoreType.DMA((DEPTH * 2,)),
                pltpu.SemaphoreType.DMA((DEPTH * 2,)),
                pltpu.SemaphoreType.DMA((2 * nch,)),
                pltpu.SemaphoreType.DMA((2 * nch,)),
                pltpu.SemaphoreType.DMA((nch,)),
                pltpu.SemaphoreType.DMA((nch,)),
                pltpu.SemaphoreType.DMA((3,)),
                pltpu.SemaphoreType.DMA((3,)),
            ],
            compiler_params=pltpu.CompilerParams(
                collective_id=0, has_side_effects=True,
                vmem_limit_bytes=40 * 1024 * 1024),
        )(in_hbm(hidden), in_hbm(final_gain.reshape(width // LANES, LANES)), in_hbm(targets),
          temperature.reshape(1), in_hbm(table_cols.T))
        keep = [pltpu.with_memory_space_constraint(a, pltpu.VMEM) for a in (pexp, peak, stat)]
        probs, ln, tl = pl.pallas_call(
            finish_kernel,
            grid=(FINISH_STEPS,),
            out_shape=(pltpu.HBM((tokens, shard), jnp.bfloat16),
                       pltpu.HBM((tokens,), f32), pltpu.HBM((tokens,), f32)),
            in_specs=[vm, vm, vm],
            out_specs=(pl.BlockSpec((tokens, nch // FINISH_STEPS * chunk), lambda i: (0, i)), vm, vm),
            compiler_params=pltpu.CompilerParams(vmem_limit_bytes=8 * 1024 * 1024),
        )(*keep)
        return ln, tl, probs

    return jax.shard_map(local_scores, mesh=mesh,
                         in_specs=(P('dp', None), P(None), P(None, 'tp'), P('dp'), P()),
                         out_specs=(P('dp'), P('dp'), P('dp', 'tp')),
                         check_vma=False)
```

```python
import math

import jax
import jax.numpy as jnp
from jax import lax
from jax.experimental import pallas as pl
from jax.experimental.pallas import tpu as pltpu
from jax.sharding import PartitionSpec as P

NORM_EPS = 1e-6
LANES = 128
LOG2E = math.log2(math.e)
LN2 = math.log(2.0)
NBLK = 7
TAIL = 3
DEPTH = 3
LAG = 2
RING = 2 * LAG + 2
GROUPS = (1, 1, 2, 4, 6, 8, 8, 6, 4, 2)
PIECES = 6
MESH = pl.DeviceIdType.MESH


def dot(u, window):
    return jnp.dot(u, window, preferred_element_type=jnp.float32)


def head_kernel(rows, vocab, tp,
                hid_hbm, gain_hbm, tgt_hbm, temp_ref, tab_ref,
                pexp_ref, ptail_ref, peak_ref, stat_ref,
                win, twin, stg, mine, part, rx, tout, tin, stat_out, stat_in, ubuf,
                hid_ref, gain_ref, tgt_ref,
                in_sem, win_sem, twin_sem, psend, precv, xsend, xrecv, tsend, trecv, ssend, srecv):
    me = lax.axis_index('tp')
    chip = me // 2
    core = me % 2
    partner = chip * 2 + (1 - core)
    across = (1 - chip) * 2 + core
    diag = (1 - chip) * 2 + (1 - core)
    peers = (across, diag, partner)
    shard = vocab // tp
    tokens, width = hid_hbm.shape
    chunk = NBLK * LANES
    nch = sum(GROUPS)
    steps = 2 * nch
    tail_at = nch * chunk
    last_blk = vocab // LANES - 1

    barrier = pltpu.get_barrier_semaphore()
    for peer in peers:
        pl.semaphore_signal(barrier, inc=1, device_id={'tp': peer}, device_id_type=MESH)

    small = [pltpu.make_async_copy(src, dst, in_sem.at[i]) for i, (src, dst) in enumerate((
        (hid_hbm, hid_ref), (gain_hbm, gain_ref), (tgt_hbm, tgt_ref)))]

    def window(g, which):
        far = g < nch
        k = jnp.where(far, g, g - nch)
        there = jnp.where(far, 1 - chip, chip)
        dest = there * 2 + (jnp.where(which == 0, 1 - core, core))
        blk = (dest * shard) // LANES + k * NBLK
        slot = (g % DEPTH) * 2 + which
        return pltpu.make_async_copy(
            tab_ref.at[:, pl.ds(pl.multiple_of(blk * LANES, LANES), chunk + LANES)],
            win.at[slot], win_sem.at[slot]), dest, slot

    def fetch(g):
        window(g, 0)[0].start()
        window(g, 1)[0].start()

    def tail_window(i, dest):
        blk = (dest * shard) // LANES + nch * NBLK
        edge = jnp.minimum(blk + TAIL, last_blk)
        for at, first, count in ((blk, 0, TAIL), (edge, TAIL, 1)):
            pltpu.make_async_copy(
                tab_ref.at[:, pl.ds(pl.multiple_of(at * LANES, LANES), count * LANES)],
                twin.at[i, :, pl.ds(first * LANES, count * LANES)], twin_sem.at[i]).start()

    tail_dests = (across, diag, partner, me)
    small[0].start()
    small[1].start()
    tail_window(0, across)
    tail_window(1, diag)
    for g in range(DEPTH):
        fetch(g)
    small[2].start()
    tail_window(2, partner)
    tail_window(3, me)
    small[0].wait()
    small[1].wait()

    x = hid_ref[...].astype(jnp.float32)
    inv_rms = lax.rsqrt(jnp.mean(x * x, axis=-1, keepdims=True) + NORM_EPS)
    gain = jnp.concatenate([gain_ref[i:i + 1] for i in range(width // LANES)], axis=1).astype(jnp.float32)
    u_all = x * inv_rms * gain
    u = u_all[:, :rows]
    for t in range(1, tp):
        u = jnp.where(me == t, u_all[:, t * rows:(t + 1) * rows], u)
    ubuf[...] = u.astype(jnp.bfloat16)

    lane = lax.broadcasted_iota(jnp.int32, (tokens, LANES), 1)
    row = lax.broadcasted_iota(jnp.int32, (tokens, LANES), 0)

    def place(z, dest, blocks, store):
        back = LANES - (dest * shard) % LANES
        rolled = [pltpu.roll(z[:, b * LANES:(b + 1) * LANES], back, 1) for b in range(blocks + 1)]
        for b in range(blocks):
            store(b, jnp.where(lane < back, rolled[b], rolled[b + 1]))

    def tail_logits(i):
        pltpu.make_async_copy(tab_ref.at[:, pl.ds(0, (TAIL + 1) * LANES)], twin.at[i], twin_sem.at[i]).wait()

        def store(b, v):
            tout[i, :, b * LANES:(b + 1) * LANES] = v
        place(dot(ubuf[...], twin[i]), tail_dests[i], TAIL, store)

    def tail_send(i):
        return pltpu.make_async_remote_copy(
            src_ref=tout.at[i], dst_ref=tin.at[i], send_sem=tsend.at[0], recv_sem=trecv.at[0],
            device_id={'tp': tail_dests[i]}, device_id_type=MESH)

    tail_logits(0)
    pl.semaphore_wait(barrier, 3)
    tail_send(0).start()
    tail_logits(1)
    tail_send(1).start()

    def to_partner(g):
        return pltpu.make_async_remote_copy(
            src_ref=stg.at[g], dst_ref=part.at[g], send_sem=psend.at[0], recv_sem=precv.at[g % RING],
            device_id={'tp': partner}, device_id_type=MESH)

    starts = [sum(GROUPS[:i]) for i in range(len(GROUPS))]

    def to_across(i):
        chunks = pl.ds(starts[i], GROUPS[i])
        return pltpu.make_async_remote_copy(
            src_ref=mine.at[chunks], dst_ref=rx.at[chunks], send_sem=xsend.at[0], recv_sem=xrecv.at[i],
            device_id={'tp': across}, device_id_type=MESH)

    def partial_logits(g, which, out):
        copy, dest, slot = window(g, which)
        copy.wait()

        def store(b, v):
            out[g, :, b * LANES:(b + 1) * LANES] = v
        place(dot(ubuf[...], win[slot]), dest, NBLK, store)

    def combine(g):
        to_partner(g).wait_recv()
        mine[g] = mine[g] + part[g]

    def step(g, _):
        partial_logits(g, 0, stg)
        to_partner(g).start()
        partial_logits(g, 1, mine)

        @pl.when(g + DEPTH < steps)
        def _():
            fetch(g + DEPTH)

        h = g - LAG

        @pl.when(h >= 0)
        def _():
            combine(h)

        for i, first in enumerate(starts):
            @pl.when(h == first + GROUPS[i] - 1)
            def _():
                to_across(i).start()
        return 0

    lax.fori_loop(0, steps, step, 0)
    tail_logits(2)
    tail_send(2).start()
    tail_logits(3)
    for h in range(steps - LAG, steps):
        combine(h)

    small[2].wait()
    factor = LOG2E / temp_ref[0]
    target = jnp.zeros((tokens, LANES), jnp.int32)
    for i in range(tokens):
        target = jnp.where(row == i, tgt_ref[i], target)
    target = target - me * shard

    def softmax_step(carry, at, ts, store):
        m, s, tg = carry
        new_m = m
        for b, t in enumerate(ts):
            tg = tg + jnp.where(lane + (at + b * LANES) == target, t, 0.0)
            new_m = jnp.maximum(new_m, t)
        s = s * jnp.exp2(m - new_m)
        for b, t in enumerate(ts):
            p = jnp.exp2(t - new_m)
            s = s + p
            store(b, p)
        return new_m, s, tg

    def absorb(k, carry):
        def store(b, p):
            pexp_ref[k, :, b * LANES:(b + 1) * LANES] = p
        ts = [(mine[nch + k, :, b * LANES:(b + 1) * LANES] + rx[k, :, b * LANES:(b + 1) * LANES]) * factor
              for b in range(NBLK)]
        carry = softmax_step(carry, k * chunk, ts, store)
        peak_ref[k] = carry[0]
        return carry

    def absorb_tail(carry):
        pltpu.make_async_copy(tin, tin, trecv.at[0]).wait()

        def store(b, p):
            ptail_ref[:, b * LANES:(b + 1) * LANES] = p
        ts = []
        for b in range(TAIL):
            cols = slice(b * LANES, (b + 1) * LANES)
            t = ((tout[3, :, cols] + tin[2, :, cols]) + (tin[0, :, cols] + tin[1, :, cols])) * factor
            ts.append(jnp.where(lane + (tail_at + b * LANES) < shard, t, -jnp.inf))
        carry = softmax_step(carry, tail_at, ts, store)
        peak_ref[nch] = carry[0]
        return carry

    zeros = jnp.zeros((tokens, LANES), jnp.float32)
    carry = (zeros - jnp.inf, zeros, zeros)
    for i, first in enumerate(starts):
        to_across(i).wait_recv()
        carry = lax.fori_loop(first, first + GROUPS[i], absorb, carry)
        if i == 0:
            carry = absorb_tail(carry)
    m, s, tg = carry

    top = jnp.max(m, axis=-1, keepdims=True)
    total = jnp.sum(s * jnp.exp2(m - top), axis=-1, keepdims=True)
    tval = jnp.sum(tg, axis=-1, keepdims=True)
    half = tokens // 2
    column = lane[:half]
    packed = jnp.zeros((half, LANES), jnp.float32)
    for i, v in enumerate((top, total, tval)):
        packed = jnp.where(column == 2 * i, v[:half], jnp.where(column == 2 * i + 1, v[half:], packed))
    stat_out[...] = packed
    sends = [pltpu.make_async_remote_copy(
        src_ref=stat_out, dst_ref=stat_in.at[i], send_sem=ssend.at[0], recv_sem=srecv.at[0],
        device_id={'tp': peer}, device_id_type=MESH) for i, peer in enumerate(peers)]
    for send in sends:
        send.start()

    pltpu.make_async_copy(stg, stg, psend.at[0]).wait()
    pltpu.make_async_copy(rx, rx, xsend.at[0]).wait()
    pltpu.make_async_copy(tin, tin, tsend.at[0]).wait()

    pltpu.make_async_copy(stat_in, stat_in, srecv.at[0]).wait()
    got = [packed] + [stat_in[i] for i in range(3)]
    for lo in range(2):
        tops = [v[:, lo:lo + 1] for v in got]
        sums = [v[:, 2 + lo:3 + lo] for v in got]
        tvals = [v[:, 4 + lo:5 + lo] for v in got]
        big = jnp.maximum(jnp.maximum(tops[0], tops[1]), jnp.maximum(tops[2], tops[3]))
        whole = sum(a * jnp.exp2(o - big) for a, o in zip(sums, tops))
        log2_norm = big + jnp.log2(whole)
        stat_ref[lo * half:(lo + 1) * half] = jnp.where(column == 0, log2_norm, sum(tvals))
    pltpu.make_async_copy(stat_in, stat_in, ssend.at[0]).wait()


def finish_kernel(pexp_ref, ptail_ref, peak_ref, stat_ref, probs_hbm, ln_hbm, tl_hbm,
                  buf, ln_buf, tl_buf, sem, vec_sem):
    tokens = stat_ref.shape[0]
    nch, _, chunk = pexp_ref.shape
    shard = buf.shape[1]
    log2_norm = stat_ref[:, 0:1]
    picked = stat_ref[:, 1:2]
    copies = []
    for j in range(PIECES):
        lo, hi = nch * j // PIECES, nch * (j + 1) // PIECES
        for k in range(lo, hi):
            scale = jnp.exp2(peak_ref[k] - log2_norm)
            for b in range(chunk // LANES):
                p = pexp_ref[k, :, b * LANES:(b + 1) * LANES] * scale
                buf[:, k * chunk + b * LANES:k * chunk + (b + 1) * LANES] = p.astype(jnp.bfloat16)
        end = hi * chunk
        if j == PIECES - 1:
            scale = jnp.exp2(peak_ref[nch] - log2_norm)
            for at in range(end, shard, LANES):
                p = (ptail_ref[:, at - end:at - end + LANES] * scale).astype(jnp.bfloat16)
                buf[:, at:min(at + LANES, shard)] = p[:, :min(LANES, shard - at)]
            end = shard
        cols = pl.ds(lo * chunk, end - lo * chunk)
        copies.append(pltpu.make_async_copy(buf.at[:, cols], probs_hbm.at[:, cols], sem.at[j]))
        copies[-1].start()
        if j == 1:
            lane = lax.broadcasted_iota(jnp.int32, (tokens, LANES), 1)
            row = lax.broadcasted_iota(jnp.int32, (tokens, LANES), 0)
            for i, (tmp, out, val) in enumerate(((ln_buf, ln_hbm, log2_norm * LN2),
                                                 (tl_buf, tl_hbm, (picked - log2_norm) * LN2))):
                tmp[...] = jnp.sum(jnp.where(row == lane, val, 0.0), axis=0)[:tokens]
                copies.append(pltpu.make_async_copy(tmp, out, vec_sem.at[i]))
                copies[-1].start()
    for copy in copies:
        copy.wait()


def solution(mesh):
    tp = mesh.shape['tp']

    def local_scores(hidden, final_gain, table_cols, targets, temperature):
        tokens, width = hidden.shape
        vocab, rows = table_cols.shape
        shard = vocab // tp
        chunk = NBLK * LANES
        nch = sum(GROUPS)
        f32, bf16 = jnp.float32, jnp.bfloat16

        def body(*refs):
            head_kernel(rows, vocab, tp, *refs)

        def in_hbm(a):
            return pltpu.with_memory_space_constraint(a, pltpu.HBM)

        def dma(n):
            return pltpu.SemaphoreType.DMA((n,))

        vm = pl.BlockSpec(memory_space=pltpu.VMEM)
        hbm = pl.BlockSpec(memory_space=pltpu.HBM)
        outs = pl.pallas_call(
            body,
            out_shape=(pltpu.VMEM((nch, tokens, chunk), f32),
                       pltpu.VMEM((tokens, TAIL * LANES), f32),
                       pltpu.VMEM((nch + 1, tokens, LANES), f32),
                       pltpu.VMEM((tokens, LANES), f32)),
            in_specs=[hbm, hbm, hbm, pl.BlockSpec(memory_space=pltpu.SMEM), hbm],
            out_specs=(vm, vm, vm, vm),
            scratch_shapes=[
                pltpu.VMEM((DEPTH * 2, rows, chunk + LANES), bf16),
                pltpu.VMEM((4, rows, (TAIL + 1) * LANES), bf16),
                pltpu.VMEM((2 * nch, tokens, chunk), f32),
                pltpu.VMEM((2 * nch, tokens, chunk), f32),
                pltpu.VMEM((2 * nch, tokens, chunk), f32),
                pltpu.VMEM((nch, tokens, chunk), f32),
                pltpu.VMEM((4, tokens, TAIL * LANES), f32),
                pltpu.VMEM((3, tokens, TAIL * LANES), f32),
                pltpu.VMEM((tokens // 2, LANES), f32),
                pltpu.VMEM((3, tokens // 2, LANES), f32),
                pltpu.VMEM((tokens, rows), bf16),
                pltpu.VMEM((tokens, width), bf16),
                pltpu.VMEM((width // LANES, LANES), bf16),
                pltpu.SMEM((tokens,), jnp.int32),
                dma(3), dma(DEPTH * 2), dma(4), dma(1), dma(RING), dma(1), dma(len(GROUPS)),
                dma(1), dma(1), dma(1), dma(1),
            ],
            compiler_params=pltpu.CompilerParams(
                collective_id=0, has_side_effects=True, vmem_limit_bytes=40 * 1024 * 1024),
        )(in_hbm(hidden), in_hbm(final_gain.reshape(width // LANES, LANES)), in_hbm(targets),
          temperature.reshape(1), in_hbm(table_cols.T))
        probs, ln, tl = pl.pallas_call(
            finish_kernel,
            out_shape=(pltpu.HBM((tokens, shard), bf16), pltpu.HBM((tokens,), f32), pltpu.HBM((tokens,), f32)),
            in_specs=[vm, vm, vm, vm],
            out_specs=(hbm, hbm, hbm),
            scratch_shapes=[
                pltpu.VMEM((tokens, shard), bf16), pltpu.VMEM((tokens,), f32), pltpu.VMEM((tokens,), f32),
                dma(PIECES), dma(2),
            ],
            compiler_params=pltpu.CompilerParams(vmem_limit_bytes=8 * 1024 * 1024),
        )(*(pltpu.with_memory_space_constraint(a, pltpu.VMEM) for a in outs))
        return ln, tl, probs

    return jax.shard_map(local_scores, mesh=mesh,
                         in_specs=(P('dp', None), P(None), P(None, 'tp'), P('dp'), P()),
                         out_specs=(P('dp'), P('dp'), P('dp', 'tp')),
                         check_vma=False)
```

```python
import math

import jax
import jax.numpy as jnp
from jax import lax
from jax.experimental import pallas as pl
from jax.experimental.pallas import tpu as pltpu
from jax.sharding import PartitionSpec as P

NORM_EPS = 1e-6
LANES = 128
LOG2E = math.log2(math.e)
LN2 = math.log(2.0)
NBLK = 7
TAIL = 3
DEPTH = 3
LAG = 2
RING = 2 * LAG + 2
GROUPS = (1, 1, 2, 4, 6, 8, 8, 6, 4, 2)
FAR = 0
HELD = 5
HOLD = 36
PIECES = 6
MESH = pl.DeviceIdType.MESH


def dot(u, window):
    return jnp.dot(u, window, preferred_element_type=jnp.float32)


def head_kernel(rows, vocab, tp,
                hid_hbm, gain_hbm, tgt_hbm, temp_ref, tab_ref,
                pexp_ref, ptail_ref, peak_ref, stat_ref,
                win, twin, stg, mine, part, rx, tout, tin, stat_out, stat_in, ubuf,
                hid_ref, gain_ref, tgt_ref,
                in_sem, win_sem, twin_sem, psend, precv, xsend, xrecv, tsend, trecv, ssend, srecv):
    me = lax.axis_index('tp')
    chip = me // 2
    core = me % 2
    partner = chip * 2 + (1 - core)
    across = (1 - chip) * 2 + core
    diag = (1 - chip) * 2 + (1 - core)
    shard = vocab // tp
    tokens, width = hid_hbm.shape
    chunk = NBLK * LANES
    nch = sum(GROUPS)
    steps = 2 * nch
    tail_at = nch * chunk
    last_blk = vocab // LANES - 1

    barrier = pltpu.get_barrier_semaphore()
    for peer in (across, diag, partner):
        pl.semaphore_signal(barrier, inc=1, device_id={'tp': peer}, device_id_type=MESH)

    small = [pltpu.make_async_copy(src, dst, in_sem.at[i]) for i, (src, dst) in enumerate((
        (hid_hbm, hid_ref), (gain_hbm, gain_ref), (tgt_hbm, tgt_ref)))]

    def window(g, which):
        far = g < nch
        k = jnp.where(far, g, g - nch)
        there = jnp.where(far, 1 - chip, chip)
        dest = there * 2 + (jnp.where(which == 0, 1 - core, core))
        blk = (dest * shard) // LANES + k * NBLK
        slot = (g % DEPTH) * 2 + which
        return pltpu.make_async_copy(
            tab_ref.at[:, pl.ds(pl.multiple_of(blk * LANES, LANES), chunk + LANES)],
            win.at[slot], win_sem.at[slot]), dest, slot

    def fetch(g):
        window(g, 0)[0].start()
        window(g, 1)[0].start()

    def tail_window(i, dest):
        blk = (dest * shard) // LANES + nch * NBLK
        edge = jnp.minimum(blk + TAIL, last_blk)
        for at, first, count in ((blk, 0, TAIL), (edge, TAIL, 1)):
            pltpu.make_async_copy(
                tab_ref.at[:, pl.ds(pl.multiple_of(at * LANES, LANES), count * LANES)],
                twin.at[i, :, pl.ds(first * LANES, count * LANES)], twin_sem.at[i]).start()

    tail_dests = (across, diag, partner, me)
    small[0].start()
    small[1].start()
    tail_window(0, across)
    tail_window(1, diag)
    for g in range(DEPTH):
        fetch(g)
    small[2].start()
    tail_window(2, partner)
    tail_window(3, me)
    small[0].wait()
    small[1].wait()

    x = hid_ref[...].astype(jnp.float32)
    inv_rms = lax.rsqrt(jnp.mean(x * x, axis=-1, keepdims=True) + NORM_EPS)
    gain = jnp.concatenate([gain_ref[i:i + 1] for i in range(width // LANES)], axis=1).astype(jnp.float32)
    u_all = x * inv_rms * gain
    u = u_all[:, :rows]
    for t in range(1, tp):
        u = jnp.where(me == t, u_all[:, t * rows:(t + 1) * rows], u)
    ubuf[...] = u.astype(jnp.bfloat16)

    lane = lax.broadcasted_iota(jnp.int32, (tokens, LANES), 1)
    row = lax.broadcasted_iota(jnp.int32, (tokens, LANES), 0)

    def place(z, dest, blocks, store):
        back = LANES - (dest * shard) % LANES
        rolled = [pltpu.roll(z[:, b * LANES:(b + 1) * LANES], back, 1) for b in range(blocks + 1)]
        for b in range(blocks):
            store(b, jnp.where(lane < back, rolled[b], rolled[b + 1]))

    def tail_logits(i):
        pltpu.make_async_copy(tab_ref.at[:, pl.ds(0, (TAIL + 1) * LANES)], twin.at[i], twin_sem.at[i]).wait()

        def store(b, v):
            tout[i, :, b * LANES:(b + 1) * LANES] = v
        place(dot(ubuf[...], twin[i]), tail_dests[i], TAIL, store)

    def tail_send(i):
        return pltpu.make_async_remote_copy(
            src_ref=tout.at[i], dst_ref=tin.at[i], send_sem=tsend.at[0], recv_sem=trecv.at[0],
            device_id={'tp': tail_dests[i]}, device_id_type=MESH)

    tail_logits(0)
    pl.semaphore_wait(barrier, 3)
    tail_send(0).start()
    tail_logits(1)
    tail_send(1).start()

    def to_partner(g):
        return pltpu.make_async_remote_copy(
            src_ref=stg.at[g], dst_ref=part.at[g], send_sem=psend.at[0], recv_sem=precv.at[g % RING],
            device_id={'tp': partner}, device_id_type=MESH)

    starts = [sum(GROUPS[:i]) for i in range(len(GROUPS))]

    def to_across(i):
        chunks = pl.ds(starts[i], GROUPS[i])
        return pltpu.make_async_remote_copy(
            src_ref=mine.at[chunks], dst_ref=rx.at[chunks], send_sem=xsend.at[0], recv_sem=xrecv.at[i],
            device_id={'tp': across}, device_id_type=MESH)

    def partial_logits(g, which, out):
        copy, dest, slot = window(g, which)
        copy.wait()

        def store(b, v):
            out[g, :, b * LANES:(b + 1) * LANES] = v
        place(dot(ubuf[...], win[slot]), dest, NBLK, store)

    def combine(g):
        to_partner(g).wait_recv()
        mine[g] = mine[g] + part[g]

    def step(g, _):
        partial_logits(g, 0, stg)
        to_partner(g).start()
        partial_logits(g, 1, mine)

        @pl.when(g + DEPTH < steps)
        def _():
            fetch(g + DEPTH)

        h = g - LAG

        @pl.when(h >= 0)
        def _():
            combine(h)

        for i, first in enumerate(starts):
            ready = first + GROUPS[i] - 1

            @pl.when(h == jnp.where(core == FAR, ready, ready if i < HELD else max(ready, HOLD)))
            def _():
                to_across(i).start()
        return 0

    lax.fori_loop(0, steps, step, 0)
    tail_logits(2)
    tail_send(2).start()
    tail_logits(3)
    for h in range(steps - LAG, steps):
        combine(h)

    small[2].wait()
    factor = LOG2E / temp_ref[0]
    target = jnp.zeros((tokens, LANES), jnp.int32)
    for i in range(tokens):
        target = jnp.where(row == i, tgt_ref[i], target)
    target = target - me * shard

    def softmax_step(carry, at, ts, store):
        m, s, tg = carry
        new_m = m
        for b, t in enumerate(ts):
            tg = tg + jnp.where(lane + (at + b * LANES) == target, t, 0.0)
            new_m = jnp.maximum(new_m, t)
        s = s * jnp.exp2(m - new_m)
        for b, t in enumerate(ts):
            p = jnp.exp2(t - new_m)
            s = s + p
            store(b, p)
        return new_m, s, tg

    def absorb(k, carry):
        def store(b, p):
            pexp_ref[k, :, b * LANES:(b + 1) * LANES] = p
        ts = [(mine[nch + k, :, b * LANES:(b + 1) * LANES] + rx[k, :, b * LANES:(b + 1) * LANES]) * factor
              for b in range(NBLK)]
        carry = softmax_step(carry, k * chunk, ts, store)
        peak_ref[k] = carry[0]
        return carry

    def absorb_tail(carry):
        pltpu.make_async_copy(tin, tin, trecv.at[0]).wait()

        def store(b, p):
            ptail_ref[:, b * LANES:(b + 1) * LANES] = p
        ts = []
        for b in range(TAIL):
            cols = slice(b * LANES, (b + 1) * LANES)
            t = ((tout[3, :, cols] + tin[2, :, cols]) + (tin[0, :, cols] + tin[1, :, cols])) * factor
            ts.append(jnp.where(lane + (tail_at + b * LANES) < shard, t, -jnp.inf))
        carry = softmax_step(carry, tail_at, ts, store)
        peak_ref[nch] = carry[0]
        return carry

    zeros = jnp.zeros((tokens, LANES), jnp.float32)
    carry = (zeros - jnp.inf, zeros, zeros)
    for i, first in enumerate(starts):
        to_across(i).wait_recv()
        carry = lax.fori_loop(first, first + GROUPS[i], absorb, carry)
        if i == 0:
            carry = absorb_tail(carry)
    m, s, tg = carry

    def stat_send(i, peer):
        return pltpu.make_async_remote_copy(
            src_ref=stat_out, dst_ref=stat_in.at[i], send_sem=ssend.at[i], recv_sem=srecv.at[i],
            device_id={'tp': peer}, device_id_type=MESH)

    def merge(a, b):
        big = jnp.maximum(a[0], b[0])
        return big, a[1] * jnp.exp2(a[0] - big) + b[1] * jnp.exp2(b[0] - big), a[2] + b[2]

    def received(i):
        stat_send(i, partner).wait_recv()
        return [stat_in[i, j] for j in range(3)]

    def put(values):
        for i, v in enumerate(values):
            stat_out[i] = v

    def conclude(stats):
        big, total, picked = stats
        top = jnp.max(big, axis=-1, keepdims=True)
        total = jnp.sum(total * jnp.exp2(big - top), axis=-1, keepdims=True)
        picked = jnp.sum(picked, axis=-1, keepdims=True)
        stat_ref[0] = jnp.broadcast_to(top + jnp.log2(total), (tokens, LANES))
        stat_ref[1] = jnp.broadcast_to(picked, (tokens, LANES))

    @pl.when(core == FAR)
    def _():
        put((m, s, tg))
        stat_send(2, partner).start()
        chip_stat = received(2)
        conclude(merge(chip_stat, received(0)))
        stat_send(2, partner).wait_send()

    @pl.when(core != FAR)
    def _():
        chip_stat = merge((m, s, tg), received(2))
        put(chip_stat)
        stat_send(0, diag).start()
        stat_send(1, across).start()
        stat_send(2, partner).start()
        conclude(merge(chip_stat, received(1)))
        for i, peer in enumerate((diag, across, partner)):
            stat_send(i, peer).wait_send()

    pltpu.make_async_copy(stg, stg, psend.at[0]).wait()
    pltpu.make_async_copy(rx, rx, xsend.at[0]).wait()
    pltpu.make_async_copy(tin, tin, tsend.at[0]).wait()


def finish_kernel(pexp_ref, ptail_ref, peak_ref, stat_ref, probs_hbm, ln_hbm, tl_hbm,
                  buf, ln_buf, tl_buf, sem, vec_sem):
    tokens = stat_ref.shape[1]
    nch, _, chunk = pexp_ref.shape
    shard = buf.shape[1]
    log2_norm = stat_ref[0]
    picked = stat_ref[1]
    copies = []
    for j in range(PIECES):
        lo, hi = nch * j // PIECES, nch * (j + 1) // PIECES
        for k in range(lo, hi):
            scale = jnp.exp2(peak_ref[k] - log2_norm)
            for b in range(chunk // LANES):
                p = pexp_ref[k, :, b * LANES:(b + 1) * LANES] * scale
                buf[:, k * chunk + b * LANES:k * chunk + (b + 1) * LANES] = p.astype(jnp.bfloat16)
        end = hi * chunk
        if j == PIECES - 1:
            scale = jnp.exp2(peak_ref[nch] - log2_norm)
            for at in range(end, shard, LANES):
                p = (ptail_ref[:, at - end:at - end + LANES] * scale).astype(jnp.bfloat16)
                buf[:, at:min(at + LANES, shard)] = p[:, :min(LANES, shard - at)]
            end = shard
        cols = pl.ds(lo * chunk, end - lo * chunk)
        copies.append(pltpu.make_async_copy(buf.at[:, cols], probs_hbm.at[:, cols], sem.at[j]))
        copies[-1].start()
        if j == 1:
            lane = lax.broadcasted_iota(jnp.int32, (tokens, LANES), 1)
            row = lax.broadcasted_iota(jnp.int32, (tokens, LANES), 0)
            for i, (tmp, out, val) in enumerate(((ln_buf, ln_hbm, log2_norm * LN2),
                                                 (tl_buf, tl_hbm, (picked - log2_norm) * LN2))):
                tmp[...] = jnp.sum(jnp.where(row == lane, val, 0.0), axis=0)[:tokens]
                copies.append(pltpu.make_async_copy(tmp, out, vec_sem.at[i]))
                copies[-1].start()
    for copy in copies:
        copy.wait()


def solution(mesh):
    tp = mesh.shape['tp']

    def local_scores(hidden, final_gain, table_cols, targets, temperature):
        tokens, width = hidden.shape
        vocab, rows = table_cols.shape
        shard = vocab // tp
        chunk = NBLK * LANES
        nch = sum(GROUPS)
        f32, bf16 = jnp.float32, jnp.bfloat16

        def body(*refs):
            head_kernel(rows, vocab, tp, *refs)

        def in_hbm(a):
            return pltpu.with_memory_space_constraint(a, pltpu.HBM)

        def dma(n):
            return pltpu.SemaphoreType.DMA((n,))

        vm = pl.BlockSpec(memory_space=pltpu.VMEM)
        hbm = pl.BlockSpec(memory_space=pltpu.HBM)
        outs = pl.pallas_call(
            body,
            out_shape=(pltpu.VMEM((nch, tokens, chunk), f32),
                       pltpu.VMEM((tokens, TAIL * LANES), f32),
                       pltpu.VMEM((nch + 1, tokens, LANES), f32),
                       pltpu.VMEM((2, tokens, LANES), f32)),
            in_specs=[hbm, hbm, hbm, pl.BlockSpec(memory_space=pltpu.SMEM), hbm],
            out_specs=(vm, vm, vm, vm),
            scratch_shapes=[
                pltpu.VMEM((DEPTH * 2, rows, chunk + LANES), bf16),
                pltpu.VMEM((4, rows, (TAIL + 1) * LANES), bf16),
                pltpu.VMEM((2 * nch, tokens, chunk), f32),
                pltpu.VMEM((2 * nch, tokens, chunk), f32),
                pltpu.VMEM((2 * nch, tokens, chunk), f32),
                pltpu.VMEM((nch, tokens, chunk), f32),
                pltpu.VMEM((4, tokens, TAIL * LANES), f32),
                pltpu.VMEM((3, tokens, TAIL * LANES), f32),
                pltpu.VMEM((3, tokens, LANES), f32),
                pltpu.VMEM((3, 3, tokens, LANES), f32),
                pltpu.VMEM((tokens, rows), bf16),
                pltpu.VMEM((tokens, width), bf16),
                pltpu.VMEM((width // LANES, LANES), bf16),
                pltpu.SMEM((tokens,), jnp.int32),
                dma(3), dma(DEPTH * 2), dma(4), dma(1), dma(RING), dma(1), dma(len(GROUPS)),
                dma(1), dma(1), dma(3), dma(3),
            ],
            compiler_params=pltpu.CompilerParams(
                collective_id=0, has_side_effects=True, vmem_limit_bytes=40 * 1024 * 1024),
        )(in_hbm(hidden), in_hbm(final_gain.reshape(width // LANES, LANES)), in_hbm(targets),
          temperature.reshape(1), in_hbm(table_cols.T))
        probs, ln, tl = pl.pallas_call(
            finish_kernel,
            out_shape=(pltpu.HBM((tokens, shard), bf16), pltpu.HBM((tokens,), f32), pltpu.HBM((tokens,), f32)),
            in_specs=[vm, vm, vm, vm],
            out_specs=(hbm, hbm, hbm),
            scratch_shapes=[
                pltpu.VMEM((tokens, shard), bf16), pltpu.VMEM((tokens,), f32), pltpu.VMEM((tokens,), f32),
                dma(PIECES), dma(2),
            ],
            compiler_params=pltpu.CompilerParams(vmem_limit_bytes=8 * 1024 * 1024),
        )(*(pltpu.with_memory_space_constraint(a, pltpu.VMEM) for a in outs))
        return ln, tl, probs

    return jax.shard_map(local_scores, mesh=mesh,
                         in_specs=(P('dp', None), P(None), P(None, 'tp'), P('dp'), P()),
                         out_specs=(P('dp'), P('dp'), P('dp', 'tp')),
                         check_vma=False)
```

```python
import math

import jax
import jax.numpy as jnp
from jax import lax
from jax.experimental import pallas as pl
from jax.experimental.pallas import tpu as pltpu
from jax.sharding import PartitionSpec as P

NORM_EPS = 1e-6
LANES = 128
LOG2E = math.log2(math.e)
LN2 = math.log(2.0)
NBLK = 7
TAIL = 3
DEPTH = 3
RING = 6
GROUPS = (1, 1, 2, 4, 6, 8, 8, 8, 3, 1)
FAR = 0
HELD = 5
HOLD = 36
PIECES = 6
MESH = pl.DeviceIdType.MESH


def dot(u, window):
    return jnp.dot(u, window, preferred_element_type=jnp.float32)


def head_kernel(rows, vocab, tp,
                hid_hbm, gain_hbm, tgt_hbm, temp_ref, tab_ref,
                pexp_ref, ptail_ref, peak_ref, stat_ref,
                win, twin, stg, mine, part, rx, tout, tin, stat_out, stat_in, ubuf,
                hid_ref, gain_ref, tgt_ref,
                in_sem, win_sem, twin_sem, psend, precv, xsend, xrecv, tsend, trecv, ssend, srecv):
    me = lax.axis_index('tp')
    chip = me // 2
    core = me % 2
    partner = chip * 2 + (1 - core)
    across = (1 - chip) * 2 + core
    diag = (1 - chip) * 2 + (1 - core)
    shard = vocab // tp
    tokens, width = hid_hbm.shape
    chunk = NBLK * LANES
    nch = sum(GROUPS)
    steps = 2 * nch
    tail_at = nch * chunk
    last_blk = vocab // LANES - 1

    barrier = pltpu.get_barrier_semaphore()
    for peer in (across, diag, partner):
        pl.semaphore_signal(barrier, inc=1, device_id={'tp': peer}, device_id_type=MESH)

    small = [pltpu.make_async_copy(src, dst, in_sem.at[i]) for i, (src, dst) in enumerate((
        (hid_hbm, hid_ref), (gain_hbm, gain_ref), (tgt_hbm, tgt_ref)))]

    def window(g, which):
        far = g < nch
        k = jnp.where(far, g, g - nch)
        there = jnp.where(far, 1 - chip, chip)
        dest = there * 2 + (jnp.where(which == 0, 1 - core, core))
        blk = (dest * shard) // LANES + k * NBLK
        slot = (g % DEPTH) * 2 + which
        return pltpu.make_async_copy(
            tab_ref.at[:, pl.ds(pl.multiple_of(blk * LANES, LANES), chunk + LANES)],
            win.at[slot], win_sem.at[slot]), dest, slot

    def fetch(g, which):
        window(g, which)[0].start()

    def tail_window(i, dest):
        blk = (dest * shard) // LANES + nch * NBLK
        edge = jnp.minimum(blk + TAIL, last_blk)
        for at, first, count in ((blk, 0, TAIL), (edge, TAIL, 1)):
            pltpu.make_async_copy(
                tab_ref.at[:, pl.ds(pl.multiple_of(at * LANES, LANES), count * LANES)],
                twin.at[i, :, pl.ds(first * LANES, count * LANES)], twin_sem.at[i]).start()

    tail_dests = (across, diag, partner, me)
    small[0].start()
    small[1].start()
    fetch(0, 0)
    tail_window(0, across)
    tail_window(1, diag)
    fetch(0, 1)
    small[0].wait()
    small[1].wait()

    x = hid_ref[...].astype(jnp.float32)
    inv_rms = lax.rsqrt(jnp.mean(x * x, axis=-1, keepdims=True) + NORM_EPS)
    gain = jnp.concatenate([gain_ref[i:i + 1] for i in range(width // LANES)], axis=1).astype(jnp.float32)
    own, own_gain = x[:, :rows], gain[:, :rows]
    for t in range(1, tp):
        cols = slice(t * rows, (t + 1) * rows)
        own = jnp.where(me == t, x[:, cols], own)
        own_gain = jnp.where(me == t, gain[:, cols], own_gain)
    ubuf[...] = (own * inv_rms * own_gain).astype(jnp.bfloat16)

    lane = lax.broadcasted_iota(jnp.int32, (tokens, LANES), 1)
    row = lax.broadcasted_iota(jnp.int32, (tokens, LANES), 0)

    def place(z, dest, blocks, store):
        back = LANES - (dest * shard) % LANES
        rolled = [pltpu.roll(z[:, b * LANES:(b + 1) * LANES], back, 1) for b in range(blocks + 1)]
        for b in range(blocks):
            store(b, jnp.where(lane < back, rolled[b], rolled[b + 1]))

    def tail_logits(i):
        pltpu.make_async_copy(tab_ref.at[:, pl.ds(0, (TAIL + 1) * LANES)], twin.at[i], twin_sem.at[i]).wait()

        def store(b, v):
            tout[i, :, b * LANES:(b + 1) * LANES] = v
        place(dot(ubuf[...], twin[i]), tail_dests[i], TAIL, store)

    def tail_send(i):
        return pltpu.make_async_remote_copy(
            src_ref=tout.at[i], dst_ref=tin.at[i], send_sem=tsend.at[0], recv_sem=trecv.at[0],
            device_id={'tp': tail_dests[i]}, device_id_type=MESH)

    def to_partner(g):
        return pltpu.make_async_remote_copy(
            src_ref=stg.at[g], dst_ref=part.at[g], send_sem=psend.at[0], recv_sem=precv.at[g % RING],
            device_id={'tp': partner}, device_id_type=MESH)

    starts = [sum(GROUPS[:i]) for i in range(len(GROUPS))]

    def to_across(i):
        chunks = pl.ds(starts[i], GROUPS[i])
        return pltpu.make_async_remote_copy(
            src_ref=mine.at[chunks], dst_ref=rx.at[chunks], send_sem=xsend.at[0], recv_sem=xrecv.at[i],
            device_id={'tp': across}, device_id_type=MESH)

    def partial_logits(g, which, out):
        copy, dest, slot = window(g, which)
        copy.wait()

        def store(b, v):
            out[g, :, b * LANES:(b + 1) * LANES] = v
        place(dot(ubuf[...], win[slot]), dest, NBLK, store)

    def combine(g):
        to_partner(g).wait_recv()
        mine[g] = mine[g] + part[g]

    def fetch_next(g, which):
        @pl.when(g + DEPTH < steps)
        def _():
            fetch(g + DEPTH, which)

    def hand_over(g):
        partial_logits(g, 0, stg)
        to_partner(g).start()
        fetch_next(g, 0)

    def keep(g):
        partial_logits(g, 1, mine)
        fetch_next(g, 1)

    partial_logits(0, 0, stg)
    fetch(1, 0)
    fetch(1, 1)
    fetch(2, 0)
    fetch(2, 1)
    small[2].start()
    tail_window(2, partner)
    tail_window(3, me)
    tail_logits(0)
    pl.semaphore_wait(barrier, 3)
    to_partner(0).start()
    tail_send(0).start()
    tail_logits(1)
    tail_send(1).start()
    fetch(DEPTH, 0)
    hand_over(1)
    keep(0)
    combine(0)
    to_across(0).start()
    hand_over(2)
    keep(1)
    combine(1)
    to_across(1).start()

    def step(g, _):
        @pl.when(g + 1 < steps)
        def _():
            hand_over(g + 1)
        keep(g)
        h = g - 1

        @pl.when(h >= 2)
        def _():
            combine(h)

        for i, first in enumerate(starts[2:], 2):
            ready = first + GROUPS[i] - 1

            @pl.when(h == jnp.where(core == FAR, ready, ready if i < HELD else max(ready, HOLD)))
            def _():
                to_across(i).start()
        return 0

    lax.fori_loop(2, steps, step, 0)
    tail_logits(2)
    tail_send(2).start()
    tail_logits(3)
    combine(steps - 1)

    small[2].wait()
    factor = LOG2E / temp_ref[0]
    target = jnp.zeros((tokens, LANES), jnp.int32)
    for i in range(tokens):
        target = jnp.where(row == i, tgt_ref[i], target)
    target = target - me * shard

    def softmax_step(carry, at, ts, store):
        m, s, tg = carry
        new_m = m
        for b, t in enumerate(ts):
            tg = tg + jnp.where(lane + (at + b * LANES) == target, t, 0.0)
            new_m = jnp.maximum(new_m, t)
        s = s * jnp.exp2(m - new_m)
        for b, t in enumerate(ts):
            p = jnp.exp2(t - new_m)
            s = s + p
            store(b, p)
        return new_m, s, tg

    def absorb(k, carry):
        def store(b, p):
            pexp_ref[k, :, b * LANES:(b + 1) * LANES] = p
        ts = [(mine[nch + k, :, b * LANES:(b + 1) * LANES] + rx[k, :, b * LANES:(b + 1) * LANES]) * factor
              for b in range(NBLK)]
        carry = softmax_step(carry, k * chunk, ts, store)
        peak_ref[k] = carry[0]
        return carry

    def absorb_tail(carry):
        pltpu.make_async_copy(tin, tin, trecv.at[0]).wait()

        def store(b, p):
            ptail_ref[:, b * LANES:(b + 1) * LANES] = p
        ts = []
        for b in range(TAIL):
            cols = slice(b * LANES, (b + 1) * LANES)
            t = ((tout[3, :, cols] + tin[2, :, cols]) + (tin[0, :, cols] + tin[1, :, cols])) * factor
            ts.append(jnp.where(lane + (tail_at + b * LANES) < shard, t, -jnp.inf))
        carry = softmax_step(carry, tail_at, ts, store)
        peak_ref[nch] = carry[0]
        return carry

    zeros = jnp.zeros((tokens, LANES), jnp.float32)
    carry = (zeros - jnp.inf, zeros, zeros)
    for i, first in enumerate(starts):
        to_across(i).wait_recv()
        carry = lax.fori_loop(first, first + GROUPS[i], absorb, carry)
        if i == 0:
            carry = absorb_tail(carry)
    m, s, tg = carry

    def stat_send(i, peer):
        return pltpu.make_async_remote_copy(
            src_ref=stat_out, dst_ref=stat_in.at[i], send_sem=ssend.at[i], recv_sem=srecv.at[i],
            device_id={'tp': peer}, device_id_type=MESH)

    def merge(a, b):
        big = jnp.maximum(a[0], b[0])
        return big, a[1] * jnp.exp2(a[0] - big) + b[1] * jnp.exp2(b[0] - big), a[2] + b[2]

    def received(i):
        stat_send(i, partner).wait_recv()
        return [stat_in[i, j] for j in range(3)]

    def put(values):
        for i, v in enumerate(values):
            stat_out[i] = v

    def conclude(stats):
        big, total, picked = stats
        top = jnp.max(big, axis=-1, keepdims=True)
        total = jnp.sum(total * jnp.exp2(big - top), axis=-1, keepdims=True)
        picked = jnp.sum(picked, axis=-1, keepdims=True)
        stat_ref[0] = jnp.broadcast_to(top + jnp.log2(total), (tokens, LANES))
        stat_ref[1] = jnp.broadcast_to(picked, (tokens, LANES))

    @pl.when(core == FAR)
    def _():
        put((m, s, tg))
        stat_send(2, partner).start()
        chip_stat = received(2)
        conclude(merge(chip_stat, received(0)))
        stat_send(2, partner).wait_send()

    @pl.when(core != FAR)
    def _():
        chip_stat = merge((m, s, tg), received(2))
        put(chip_stat)
        stat_send(0, diag).start()
        stat_send(1, across).start()
        stat_send(2, partner).start()
        conclude(merge(chip_stat, received(1)))
        for i, peer in enumerate((diag, across, partner)):
            stat_send(i, peer).wait_send()

    pltpu.make_async_copy(stg, stg, psend.at[0]).wait()
    pltpu.make_async_copy(rx, rx, xsend.at[0]).wait()
    pltpu.make_async_copy(tin, tin, tsend.at[0]).wait()


def finish_kernel(pexp_ref, ptail_ref, peak_ref, stat_ref, probs_hbm, ln_hbm, tl_hbm,
                  buf, ln_buf, tl_buf, sem, vec_sem):
    tokens = stat_ref.shape[1]
    nch, _, chunk = pexp_ref.shape
    shard = buf.shape[1]
    log2_norm = stat_ref[0]
    picked = stat_ref[1]
    copies = []
    for j in range(PIECES):
        lo, hi = nch * j // PIECES, nch * (j + 1) // PIECES
        for k in range(lo, hi):
            scale = jnp.exp2(peak_ref[k] - log2_norm)
            for b in range(chunk // LANES):
                p = pexp_ref[k, :, b * LANES:(b + 1) * LANES] * scale
                buf[:, k * chunk + b * LANES:k * chunk + (b + 1) * LANES] = p.astype(jnp.bfloat16)
        end = hi * chunk
        if j == PIECES - 1:
            scale = jnp.exp2(peak_ref[nch] - log2_norm)
            for at in range(end, shard, LANES):
                p = (ptail_ref[:, at - end:at - end + LANES] * scale).astype(jnp.bfloat16)
                buf[:, at:min(at + LANES, shard)] = p[:, :min(LANES, shard - at)]
            end = shard
        cols = pl.ds(lo * chunk, end - lo * chunk)
        copies.append(pltpu.make_async_copy(buf.at[:, cols], probs_hbm.at[:, cols], sem.at[j]))
        copies[-1].start()
        if j == 1:
            lane = lax.broadcasted_iota(jnp.int32, (tokens, LANES), 1)
            row = lax.broadcasted_iota(jnp.int32, (tokens, LANES), 0)
            for i, (tmp, out, val) in enumerate(((ln_buf, ln_hbm, log2_norm * LN2),
                                                 (tl_buf, tl_hbm, (picked - log2_norm) * LN2))):
                tmp[...] = jnp.sum(jnp.where(row == lane, val, 0.0), axis=0)[:tokens]
                copies.append(pltpu.make_async_copy(tmp, out, vec_sem.at[i]))
                copies[-1].start()
    for copy in copies:
        copy.wait()


def solution(mesh):
    tp = mesh.shape['tp']

    def local_scores(hidden, final_gain, table_cols, targets, temperature):
        tokens, width = hidden.shape
        vocab, rows = table_cols.shape
        shard = vocab // tp
        chunk = NBLK * LANES
        nch = sum(GROUPS)
        f32, bf16 = jnp.float32, jnp.bfloat16

        def body(*refs):
            head_kernel(rows, vocab, tp, *refs)

        def in_hbm(a):
            return pltpu.with_memory_space_constraint(a, pltpu.HBM)

        def dma(n):
            return pltpu.SemaphoreType.DMA((n,))

        vm = pl.BlockSpec(memory_space=pltpu.VMEM)
        hbm = pl.BlockSpec(memory_space=pltpu.HBM)
        outs = pl.pallas_call(
            body,
            out_shape=(pltpu.VMEM((nch, tokens, chunk), f32),
                       pltpu.VMEM((tokens, TAIL * LANES), f32),
                       pltpu.VMEM((nch + 1, tokens, LANES), f32),
                       pltpu.VMEM((2, tokens, LANES), f32)),
            in_specs=[hbm, hbm, hbm, pl.BlockSpec(memory_space=pltpu.SMEM), hbm],
            out_specs=(vm, vm, vm, vm),
            scratch_shapes=[
                pltpu.VMEM((DEPTH * 2, rows, chunk + LANES), bf16),
                pltpu.VMEM((4, rows, (TAIL + 1) * LANES), bf16),
                pltpu.VMEM((2 * nch, tokens, chunk), f32),
                pltpu.VMEM((2 * nch, tokens, chunk), f32),
                pltpu.VMEM((2 * nch, tokens, chunk), f32),
                pltpu.VMEM((nch, tokens, chunk), f32),
                pltpu.VMEM((4, tokens, TAIL * LANES), f32),
                pltpu.VMEM((3, tokens, TAIL * LANES), f32),
                pltpu.VMEM((3, tokens, LANES), f32),
                pltpu.VMEM((3, 3, tokens, LANES), f32),
                pltpu.VMEM((tokens, rows), bf16),
                pltpu.VMEM((tokens, width), bf16),
                pltpu.VMEM((width // LANES, LANES), bf16),
                pltpu.SMEM((tokens,), jnp.int32),
                dma(3), dma(DEPTH * 2), dma(4), dma(1), dma(RING), dma(1), dma(len(GROUPS)),
                dma(1), dma(1), dma(3), dma(3),
            ],
            compiler_params=pltpu.CompilerParams(
                collective_id=0, has_side_effects=True, vmem_limit_bytes=40 * 1024 * 1024),
        )(in_hbm(hidden), in_hbm(final_gain.reshape(width // LANES, LANES)), in_hbm(targets),
          temperature.reshape(1), in_hbm(table_cols.T))
        probs, ln, tl = pl.pallas_call(
            finish_kernel,
            out_shape=(pltpu.HBM((tokens, shard), bf16), pltpu.HBM((tokens,), f32), pltpu.HBM((tokens,), f32)),
            in_specs=[vm, vm, vm, vm],
            out_specs=(hbm, hbm, hbm),
            scratch_shapes=[
                pltpu.VMEM((tokens, shard), bf16), pltpu.VMEM((tokens,), f32), pltpu.VMEM((tokens,), f32),
                dma(PIECES), dma(2),
            ],
            compiler_params=pltpu.CompilerParams(vmem_limit_bytes=8 * 1024 * 1024),
        )(*(pltpu.with_memory_space_constraint(a, pltpu.VMEM) for a in outs))
        return ln, tl, probs

    return jax.shard_map(local_scores, mesh=mesh,
                         in_specs=(P('dp', None), P(None), P(None, 'tp'), P('dp'), P()),
                         out_specs=(P('dp'), P('dp'), P('dp', 'tp')),
                         check_vma=False)
```

```python
import math

import jax
import jax.numpy as jnp
from jax import lax
from jax.experimental import pallas as pl
from jax.experimental.pallas import tpu as pltpu
from jax.sharding import PartitionSpec as P

NORM_EPS = 1e-6
LANES = 128
LOG2E = math.log2(math.e)
LN2 = math.log(2.0)
NBLK = 7
TAIL = 3
DEPTH = 3
RING = 6
GROUPS = (1, 1, 2, 4, 6, 8, 8, 8, 3, 1)
FAR = 0
HELD = 5
HOLD = 36
JOINT = (7, 8, 9, 10)
PIECES = 6
MESH = pl.DeviceIdType.MESH


def dot(u, window):
    return jnp.dot(u, window, preferred_element_type=jnp.float32)


def head_kernel(rows, vocab, tp,
                hid_hbm, gain_hbm, tgt_hbm, temp_ref, tab_ref,
                pexp_ref, ptail_ref, peak_ref, stat_ref,
                win, twin, stg, mine, part, rx, tout, tin, stat_out, stat_in, stat_all, ubuf,
                hid_ref, gain_ref, tgt_ref,
                in_sem, win_sem, twin_sem, psend, precv, xsend, xrecv, tsend, trecv, ssend, srecv, go):
    me = lax.axis_index('tp')
    chip = me // 2
    core = me % 2
    partner = chip * 2 + (1 - core)
    across = (1 - chip) * 2 + core
    diag = (1 - chip) * 2 + (1 - core)
    shard = vocab // tp
    tokens, width = hid_hbm.shape
    chunk = NBLK * LANES
    nch = sum(GROUPS)
    steps = 2 * nch
    tail_at = nch * chunk
    last_blk = vocab // LANES - 1

    barrier = pltpu.get_barrier_semaphore()
    for peer in (partner, diag):
        pl.semaphore_signal(barrier, inc=1, device_id={'tp': peer}, device_id_type=MESH)

    @pl.when(core != FAR)
    def _():
        pl.semaphore_signal(barrier, inc=1, device_id={'tp': across}, device_id_type=MESH)


    small = [pltpu.make_async_copy(src, dst, in_sem.at[i]) for i, (src, dst) in enumerate((
        (hid_hbm, hid_ref), (gain_hbm, gain_ref), (tgt_hbm, tgt_ref)))]

    def window(g, which):
        far = g < nch
        k = jnp.where(far, g, g - nch)
        there = jnp.where(far, 1 - chip, chip)
        dest = there * 2 + (jnp.where(which == 0, 1 - core, core))
        blk = (dest * shard) // LANES + k * NBLK
        slot = (g % DEPTH) * 2 + which
        return pltpu.make_async_copy(
            tab_ref.at[:, pl.ds(pl.multiple_of(blk * LANES, LANES), chunk + LANES)],
            win.at[slot], win_sem.at[slot]), dest, slot

    def fetch(g, which):
        window(g, which)[0].start()

    def tail_window(i, dest):
        blk = (dest * shard) // LANES + nch * NBLK
        edge = jnp.minimum(blk + TAIL, last_blk)
        for at, first, count in ((blk, 0, TAIL), (edge, TAIL, 1)):
            pltpu.make_async_copy(
                tab_ref.at[:, pl.ds(pl.multiple_of(at * LANES, LANES), count * LANES)],
                twin.at[i % 2, :, pl.ds(first * LANES, count * LANES)], twin_sem.at[i % 2]).start()

    tail_dests = ((1 - chip) * 2 + (1 - FAR), (1 - chip) * 2 + FAR, partner, me)
    small[0].start()
    small[1].start()
    fetch(0, 0)
    tail_window(0, tail_dests[0])
    tail_window(1, tail_dests[1])
    fetch(0, 1)
    small[0].wait()
    small[1].wait()

    x = hid_ref[...].astype(jnp.float32)
    inv_rms = lax.rsqrt(jnp.mean(x * x, axis=-1, keepdims=True) + NORM_EPS)
    gain = jnp.concatenate([gain_ref[i:i + 1] for i in range(width // LANES)], axis=1).astype(jnp.float32)
    own, own_gain = x[:, :rows], gain[:, :rows]
    for t in range(1, tp):
        cols = slice(t * rows, (t + 1) * rows)
        own = jnp.where(me == t, x[:, cols], own)
        own_gain = jnp.where(me == t, gain[:, cols], own_gain)
    ubuf[...] = (own * inv_rms * own_gain).astype(jnp.bfloat16)

    lane = lax.broadcasted_iota(jnp.int32, (tokens, LANES), 1)
    row = lax.broadcasted_iota(jnp.int32, (tokens, LANES), 0)

    def place(z, dest, blocks, store):
        back = LANES - (dest * shard) % LANES
        rolled = [pltpu.roll(z[:, b * LANES:(b + 1) * LANES], back, 1) for b in range(blocks + 1)]
        for b in range(blocks):
            store(b, jnp.where(lane < back, rolled[b], rolled[b + 1]))

    def tail_logits(i):
        pltpu.make_async_copy(tab_ref.at[:, pl.ds(0, (TAIL + 1) * LANES)], twin.at[i % 2], twin_sem.at[i % 2]).wait()

        def store(b, v):
            tout[i, :, b * LANES:(b + 1) * LANES] = v
        place(dot(ubuf[...], twin[i % 2]), tail_dests[i], TAIL, store)

    def tail_send(i):
        slot = 2 if i == 2 else (jnp.where(core == FAR, 1 - i, i))
        return pltpu.make_async_remote_copy(
            src_ref=tout.at[i], dst_ref=tin.at[slot], send_sem=tsend.at[0], recv_sem=trecv.at[0],
            device_id={'tp': tail_dests[i]}, device_id_type=MESH)

    def to_partner(g):
        return pltpu.make_async_remote_copy(
            src_ref=stg.at[g], dst_ref=part.at[g], send_sem=psend.at[0], recv_sem=precv.at[g % RING],
            device_id={'tp': partner}, device_id_type=MESH)

    starts = [sum(GROUPS[:i]) for i in range(len(GROUPS))]

    def owner(i):
        return sum(i >= end for end in JOINT[:-1])

    def to_across(i):
        chunks = pl.ds(starts[i], GROUPS[i])
        return pltpu.make_async_remote_copy(
            src_ref=mine.at[chunks], dst_ref=rx.at[chunks], send_sem=xsend.at[0], recv_sem=xrecv.at[owner(i)],
            device_id={'tp': across}, device_id_type=MESH)

    def partial_logits(g, which, out):
        copy, dest, slot = window(g, which)
        copy.wait()

        def store(b, v):
            out[g, :, b * LANES:(b + 1) * LANES] = v
        place(dot(ubuf[...], win[slot]), dest, NBLK, store)

    def combine(g):
        to_partner(g).wait_recv()
        mine[g] = mine[g] + part[g]

    def fetch_next(g, which):
        @pl.when(g + DEPTH < steps)
        def _():
            fetch(g + DEPTH, which)

    def hand_over(g):
        partial_logits(g, 0, stg)
        to_partner(g).start()
        fetch_next(g, 0)

    def keep(g):
        partial_logits(g, 1, mine)
        fetch_next(g, 1)

    partial_logits(0, 0, stg)
    fetch(1, 0)
    fetch(1, 1)
    fetch(2, 0)
    fetch(2, 1)
    small[2].start()
    tail_logits(0)

    @pl.when(core == FAR)
    def _():
        pl.semaphore_wait(barrier, 2)

    @pl.when(core != FAR)
    def _():
        pl.semaphore_wait(barrier, 3)
        pl.semaphore_signal(go, inc=1, device_id={'tp': partner}, device_id_type=MESH)

    to_partner(0).start()
    tail_send(0).start()
    tail_logits(1)

    @pl.when(core == FAR)
    def _():
        pl.semaphore_wait(go, 1)

    tail_send(1).start()
    fetch(DEPTH, 0)
    hand_over(1)
    keep(0)
    combine(0)
    to_across(0).start()
    hand_over(2)
    keep(1)
    combine(1)
    to_across(1).start()
    tail_window(2, partner)
    tail_window(3, me)

    def step(g, _):
        @pl.when(g + 1 < steps)
        def _():
            hand_over(g + 1)
        keep(g)
        h = g - 1

        @pl.when(h >= 2)
        def _():
            combine(h)

        for i, first in enumerate(starts[2:], 2):
            ready = first + GROUPS[i] - 1

            @pl.when(h == jnp.where(core == FAR, ready, ready if i < HELD else max(ready, HOLD)))
            def _():
                to_across(i).start()
        return 0

    lax.fori_loop(2, steps, step, 0)
    tail_logits(2)
    tail_send(2).start()
    tail_logits(3)
    combine(steps - 1)

    small[2].wait()
    factor = LOG2E / temp_ref[0]
    target = jnp.zeros((tokens, LANES), jnp.int32)
    for i in range(tokens):
        target = jnp.where(row == i, tgt_ref[i], target)
    target = target - me * shard

    def softmax_step(carry, at, ts, store):
        m, s, tg = carry
        new_m = m
        for b, t in enumerate(ts):
            tg = tg + jnp.where(lane + (at + b * LANES) == target, t, 0.0)
            new_m = jnp.maximum(new_m, t)
        s = s * jnp.exp2(m - new_m)
        for b, t in enumerate(ts):
            p = jnp.exp2(t - new_m)
            s = s + p
            store(b, p)
        return new_m, s, tg

    def absorb(k, carry):
        def store(b, p):
            pexp_ref[k, :, b * LANES:(b + 1) * LANES] = p
        ts = [(mine[nch + k, :, b * LANES:(b + 1) * LANES] + rx[k, :, b * LANES:(b + 1) * LANES]) * factor
              for b in range(NBLK)]
        carry = softmax_step(carry, k * chunk, ts, store)
        peak_ref[k] = carry[0]
        return carry

    def absorb_tail(carry):
        pltpu.make_async_copy(tin, tin, trecv.at[0]).wait()

        def store(b, p):
            ptail_ref[:, b * LANES:(b + 1) * LANES] = p
        ts = []
        for b in range(TAIL):
            cols = slice(b * LANES, (b + 1) * LANES)
            t = ((tout[3, :, cols] + tin[2, :, cols]) + (tin[0, :, cols] + tin[1, :, cols])) * factor
            ts.append(jnp.where(lane + (tail_at + b * LANES) < shard, t, -jnp.inf))
        carry = softmax_step(carry, tail_at, ts, store)
        peak_ref[nch] = carry[0]
        return carry

    zeros = jnp.zeros((tokens, LANES), jnp.float32)
    carry = (zeros - jnp.inf, zeros, zeros)
    for j, end in enumerate(JOINT):
        begin = JOINT[j - 1] if j else 0
        first, count = starts[begin], sum(GROUPS[begin:end])
        arrived = rx.at[pl.ds(first, count)]
        pltpu.make_async_copy(arrived, arrived, xrecv.at[j]).wait()
        carry = lax.fori_loop(first, first + count, absorb, carry)
        if j == 0:
            carry = absorb_tail(carry)
    m, s, tg = carry

    def stat_send(i, peer):
        return pltpu.make_async_remote_copy(
            src_ref=stat_out, dst_ref=stat_in.at[i], send_sem=ssend.at[0], recv_sem=srecv.at[i],
            device_id={'tp': peer}, device_id_type=MESH)

    def merge(a, b):
        big = jnp.maximum(a[0], b[0])
        return big, a[1] * jnp.exp2(a[0] - big) + b[1] * jnp.exp2(b[0] - big), a[2] + b[2]

    third = LANES // 4

    def received(i):
        stat_send(i, partner).wait_recv()
        return [jnp.broadcast_to(stat_in[i, :, j * third:j * third + 1], (tokens, LANES)) for j in range(3)]

    def put(values):
        top, total, picked = values
        stat_out[...] = jnp.where(lane < third, top, jnp.where(lane < 2 * third, total, picked))

    def conclude(stats):
        big, total, picked = stats
        stat_ref[0] = big + jnp.log2(total)
        stat_ref[1] = picked

    top = jnp.max(m, axis=-1, keepdims=True)
    total = jnp.sum(s * jnp.exp2(m - top), axis=-1, keepdims=True)
    picked = jnp.sum(tg, axis=-1, keepdims=True)
    own_stat = [jnp.broadcast_to(v, (tokens, LANES)) for v in (top, total, picked)]

    @pl.when(core == FAR)
    def _():
        put(own_stat)
        stat_send(1, partner).start()
        chip_stat = received(1)
        conclude(merge(chip_stat, received(0)))
        stat_send(1, partner).wait_send()

    @pl.when(core != FAR)
    def _():
        chip_stat = merge(own_stat, received(1))
        put(chip_stat)
        stat_send(0, diag).start()
        stat_send(0, across).start()
        stat_send(1, partner).start()
        conclude(merge(chip_stat, received(0)))
        pltpu.make_async_copy(stat_all, stat_all, ssend.at[0]).wait()

    pltpu.make_async_copy(stg, stg, psend.at[0]).wait()
    pltpu.make_async_copy(rx, rx, xsend.at[0]).wait()
    pltpu.make_async_copy(tin, tin, tsend.at[0]).wait()


def finish_kernel(pexp_ref, ptail_ref, peak_ref, stat_ref, probs_hbm, ln_hbm, tl_hbm,
                  buf, ln_buf, tl_buf, sem, vec_sem):
    tokens = stat_ref.shape[1]
    nch, _, chunk = pexp_ref.shape
    shard = buf.shape[1]
    log2_norm = stat_ref[0]
    picked = stat_ref[1]
    copies = []
    for j in range(PIECES):
        lo, hi = nch * j // PIECES, nch * (j + 1) // PIECES
        for k in range(lo, hi):
            scale = jnp.exp2(peak_ref[k] - log2_norm)
            for b in range(chunk // LANES):
                p = pexp_ref[k, :, b * LANES:(b + 1) * LANES] * scale
                buf[:, k * chunk + b * LANES:k * chunk + (b + 1) * LANES] = p.astype(jnp.bfloat16)
        end = hi * chunk
        if j == PIECES - 1:
            scale = jnp.exp2(peak_ref[nch] - log2_norm)
            for at in range(end, shard, LANES):
                p = (ptail_ref[:, at - end:at - end + LANES] * scale).astype(jnp.bfloat16)
                buf[:, at:min(at + LANES, shard)] = p[:, :min(LANES, shard - at)]
            end = shard
        cols = pl.ds(lo * chunk, end - lo * chunk)
        copies.append(pltpu.make_async_copy(buf.at[:, cols], probs_hbm.at[:, cols], sem.at[j]))
        copies[-1].start()
        if j == 1:
            lane = lax.broadcasted_iota(jnp.int32, (tokens, LANES), 1)
            row = lax.broadcasted_iota(jnp.int32, (tokens, LANES), 0)
            for i, (tmp, out, val) in enumerate(((ln_buf, ln_hbm, log2_norm * LN2),
                                                 (tl_buf, tl_hbm, (picked - log2_norm) * LN2))):
                tmp[...] = jnp.sum(jnp.where(row == lane, val, 0.0), axis=0)[:tokens]
                copies.append(pltpu.make_async_copy(tmp, out, vec_sem.at[i]))
                copies[-1].start()
    for copy in copies:
        copy.wait()


def solution(mesh):
    tp = mesh.shape['tp']

    def local_scores(hidden, final_gain, table_cols, targets, temperature):
        tokens, width = hidden.shape
        vocab, rows = table_cols.shape
        shard = vocab // tp
        chunk = NBLK * LANES
        nch = sum(GROUPS)
        f32, bf16 = jnp.float32, jnp.bfloat16

        def body(*refs):
            head_kernel(rows, vocab, tp, *refs)

        def in_hbm(a):
            return pltpu.with_memory_space_constraint(a, pltpu.HBM)

        def dma(n):
            return pltpu.SemaphoreType.DMA((n,))

        vm = pl.BlockSpec(memory_space=pltpu.VMEM)
        hbm = pl.BlockSpec(memory_space=pltpu.HBM)
        outs = pl.pallas_call(
            body,
            out_shape=(pltpu.VMEM((nch, tokens, chunk), f32),
                       pltpu.VMEM((tokens, TAIL * LANES), f32),
                       pltpu.VMEM((nch + 1, tokens, LANES), f32),
                       pltpu.VMEM((2, tokens, LANES), f32)),
            in_specs=[hbm, hbm, hbm, pl.BlockSpec(memory_space=pltpu.SMEM), hbm],
            out_specs=(vm, vm, vm, vm),
            scratch_shapes=[
                pltpu.VMEM((DEPTH * 2, rows, chunk + LANES), bf16),
                pltpu.VMEM((2, rows, (TAIL + 1) * LANES), bf16),
                pltpu.VMEM((2 * nch, tokens, chunk), f32),
                pltpu.VMEM((2 * nch, tokens, chunk), f32),
                pltpu.VMEM((2 * nch, tokens, chunk), f32),
                pltpu.VMEM((nch, tokens, chunk), f32),
                pltpu.VMEM((4, tokens, TAIL * LANES), f32),
                pltpu.VMEM((3, tokens, TAIL * LANES), f32),
                pltpu.VMEM((tokens, LANES), f32),
                pltpu.VMEM((2, tokens, LANES), f32),
                pltpu.VMEM((3, tokens, LANES), f32),
                pltpu.VMEM((tokens, rows), bf16),
                pltpu.VMEM((tokens, width), bf16),
                pltpu.VMEM((width // LANES, LANES), bf16),
                pltpu.SMEM((tokens,), jnp.int32),
                dma(3), dma(DEPTH * 2), dma(2), dma(1), dma(RING), dma(1), dma(len(JOINT)),
                dma(1), dma(1), dma(1), dma(2), pltpu.SemaphoreType.REGULAR,
            ],
            compiler_params=pltpu.CompilerParams(
                collective_id=0, has_side_effects=True, vmem_limit_bytes=40 * 1024 * 1024),
        )(in_hbm(hidden), in_hbm(final_gain.reshape(width // LANES, LANES)), in_hbm(targets),
          temperature.reshape(1), in_hbm(table_cols.T))
        probs, ln, tl = pl.pallas_call(
            finish_kernel,
            out_shape=(pltpu.HBM((tokens, shard), bf16), pltpu.HBM((tokens,), f32), pltpu.HBM((tokens,), f32)),
            in_specs=[vm, vm, vm, vm],
            out_specs=(hbm, hbm, hbm),
            scratch_shapes=[
                pltpu.VMEM((tokens, shard), bf16), pltpu.VMEM((tokens,), f32), pltpu.VMEM((tokens,), f32),
                dma(PIECES), dma(2),
            ],
            compiler_params=pltpu.CompilerParams(vmem_limit_bytes=8 * 1024 * 1024),
        )(*(pltpu.with_memory_space_constraint(a, pltpu.VMEM) for a in outs))
        return ln, tl, probs

    return jax.shard_map(local_scores, mesh=mesh,
                         in_specs=(P('dp', None), P(None), P(None, 'tp'), P('dp'), P()),
                         out_specs=(P('dp'), P('dp'), P('dp', 'tp')),
                         check_vma=False)
```

```python
import jax
import jax.numpy as jnp
from jax import lax
from jax.experimental import pallas as pl
from jax.experimental.pallas import tpu as pltpu
from jax.sharding import PartitionSpec as P

NORM_EPS = 1e-6
LANES = 128
NBLK = 7
TAIL = 3
DEPTH = 3
RING = 6
GROUPS = (1, 1, 2, 4, 6, 8, 8, 8, 3, 1)
FAR = 0
HELD = 5
HOLD = 36
JOINT = (7, 8, 9, 10)
PIECES = 6
MESH = pl.DeviceIdType.MESH


def dot(u, window):
    return jnp.dot(u, window, preferred_element_type=jnp.float32)


def head_kernel(rows, vocab, tp,
                hid_hbm, gain_hbm, tgt_hbm, temp_ref, tab_ref,
                pexp_ref, ptail_ref, peak_ref, stat_ref,
                win, twin, stg, mine, part, rx, tout, tin, stat_out, stat_in, stat_all, ubuf,
                hid_ref, gain_ref, tgt_ref,
                in_sem, win_sem, twin_sem, psend, precv, xsend, xrecv, tsend, trecv, ssend, srecv, go):
    me = lax.axis_index('tp')
    chip = me // 2
    core = me % 2
    partner = chip * 2 + (1 - core)
    across = (1 - chip) * 2 + core
    diag = (1 - chip) * 2 + (1 - core)
    shard = vocab // tp
    tokens, width = hid_hbm.shape
    chunk = NBLK * LANES
    nch = sum(GROUPS)
    steps = 2 * nch
    tail_at = nch * chunk
    last_blk = vocab // LANES - 1

    barrier = pltpu.get_barrier_semaphore()
    for peer in (partner, diag):
        pl.semaphore_signal(barrier, inc=1, device_id={'tp': peer}, device_id_type=MESH)

    @pl.when(core != FAR)
    def _():
        pl.semaphore_signal(barrier, inc=1, device_id={'tp': across}, device_id_type=MESH)

    small = [pltpu.make_async_copy(src, dst, in_sem.at[i]) for i, (src, dst) in enumerate((
        (hid_hbm, hid_ref), (gain_hbm, gain_ref), (tgt_hbm, tgt_ref)))]

    def window(g, which):
        far = g < nch
        k = jnp.where(far, g, g - nch)
        there = jnp.where(far, 1 - chip, chip)
        dest = there * 2 + (jnp.where(which == 0, 1 - core, core))
        blk = (dest * shard) // LANES + k * NBLK
        slot = (g % DEPTH) * 2 + which
        return pltpu.make_async_copy(
            tab_ref.at[:, pl.ds(pl.multiple_of(blk * LANES, LANES), chunk + LANES)],
            win.at[slot], win_sem.at[slot]), dest, slot

    def fetch(g, which):
        window(g, which)[0].start()

    def tail_window(i, dest):
        blk = (dest * shard) // LANES + nch * NBLK
        edge = jnp.minimum(blk + TAIL, last_blk)
        for at, first, count in ((blk, 0, TAIL), (edge, TAIL, 1)):
            pltpu.make_async_copy(
                tab_ref.at[:, pl.ds(pl.multiple_of(at * LANES, LANES), count * LANES)],
                twin.at[i % 2, :, pl.ds(first * LANES, count * LANES)], twin_sem.at[i % 2]).start()

    tail_dests = ((1 - chip) * 2 + (1 - FAR), (1 - chip) * 2 + FAR, partner, me)
    small[0].start()
    small[1].start()
    fetch(0, 0)
    tail_window(0, tail_dests[0])
    tail_window(1, tail_dests[1])
    fetch(0, 1)
    small[0].wait()
    small[1].wait()

    x = hid_ref[...].astype(jnp.float32)
    inv_rms = lax.rsqrt(jnp.mean(x * x, axis=-1, keepdims=True) + NORM_EPS)
    gain = jnp.concatenate([gain_ref[i:i + 1] for i in range(width // LANES)], axis=1).astype(jnp.float32)
    own, own_gain = x[:, :rows], gain[:, :rows]
    for t in range(1, tp):
        cols = slice(t * rows, (t + 1) * rows)
        own = jnp.where(me == t, x[:, cols], own)
        own_gain = jnp.where(me == t, gain[:, cols], own_gain)
    ubuf[...] = (own * inv_rms * own_gain).astype(jnp.bfloat16)

    lane = lax.broadcasted_iota(jnp.int32, (tokens, LANES), 1)
    row = lax.broadcasted_iota(jnp.int32, (tokens, LANES), 0)

    def place(z, dest, blocks, store):
        back = LANES - (dest * shard) % LANES
        rolled = [pltpu.roll(z[:, b * LANES:(b + 1) * LANES], back, 1) for b in range(blocks + 1)]
        for b in range(blocks):
            store(b, jnp.where(lane < back, rolled[b], rolled[b + 1]))

    def tail_logits(i):
        pltpu.make_async_copy(tab_ref.at[:, pl.ds(0, (TAIL + 1) * LANES)], twin.at[i % 2], twin_sem.at[i % 2]).wait()

        def store(b, v):
            tout[i, :, b * LANES:(b + 1) * LANES] = v
        place(dot(ubuf[...], twin[i % 2]), tail_dests[i], TAIL, store)

    def tail_send(i):
        slot = 2 if i == 2 else (jnp.where(core == FAR, 1 - i, i))
        return pltpu.make_async_remote_copy(
            src_ref=tout.at[i], dst_ref=tin.at[slot], send_sem=tsend.at[0], recv_sem=trecv.at[0],
            device_id={'tp': tail_dests[i]}, device_id_type=MESH)

    def to_partner(g):
        return pltpu.make_async_remote_copy(
            src_ref=stg.at[g], dst_ref=part.at[g], send_sem=psend.at[0], recv_sem=precv.at[g % RING],
            device_id={'tp': partner}, device_id_type=MESH)

    starts = [sum(GROUPS[:i]) for i in range(len(GROUPS))]

    def owner(i):
        return sum(i >= end for end in JOINT[:-1])

    def to_across(i):
        chunks = pl.ds(starts[i], GROUPS[i])
        return pltpu.make_async_remote_copy(
            src_ref=mine.at[chunks], dst_ref=rx.at[chunks], send_sem=xsend.at[0], recv_sem=xrecv.at[owner(i)],
            device_id={'tp': across}, device_id_type=MESH)

    def partial_logits(g, which, out):
        copy, dest, slot = window(g, which)
        copy.wait()

        def store(b, v):
            out[g, :, b * LANES:(b + 1) * LANES] = v
        place(dot(ubuf[...], win[slot]), dest, NBLK, store)

    def combine(g):
        to_partner(g).wait_recv()
        mine[g] = mine[g] + part[g]

    def fetch_next(g, which):
        @pl.when(g + DEPTH < steps)
        def _():
            fetch(g + DEPTH, which)

    def hand_over(g):
        partial_logits(g, 0, stg)
        to_partner(g).start()
        fetch_next(g, 0)

    def keep(g):
        partial_logits(g, 1, mine)
        fetch_next(g, 1)

    partial_logits(0, 0, stg)
    fetch(1, 0)
    fetch(1, 1)
    fetch(2, 0)
    fetch(2, 1)
    small[2].start()
    tail_logits(0)

    @pl.when(core == FAR)
    def _():
        pl.semaphore_wait(barrier, 2)

    @pl.when(core != FAR)
    def _():
        pl.semaphore_wait(barrier, 3)
        pl.semaphore_signal(go, inc=1, device_id={'tp': partner}, device_id_type=MESH)

    to_partner(0).start()
    tail_send(0).start()
    tail_logits(1)

    @pl.when(core == FAR)
    def _():
        pl.semaphore_wait(go, 1)

    tail_send(1).start()
    fetch(DEPTH, 0)
    hand_over(1)
    keep(0)
    combine(0)
    to_across(0).start()
    hand_over(2)
    keep(1)
    combine(1)
    to_across(1).start()
    tail_window(2, partner)
    tail_window(3, me)

    def step(g, _):
        @pl.when(g + 1 < steps)
        def _():
            hand_over(g + 1)
        keep(g)
        h = g - 1

        @pl.when(h >= 2)
        def _():
            combine(h)

        for i, first in enumerate(starts[2:], 2):
            ready = first + GROUPS[i] - 1

            @pl.when(h == jnp.where(core == FAR, ready, ready if i < HELD else max(ready, HOLD)))
            def _():
                to_across(i).start()
        return 0

    lax.fori_loop(2, steps, step, 0)
    tail_logits(2)
    tail_send(2).start()
    tail_logits(3)
    combine(steps - 1)

    small[2].wait()
    factor = 1.0 / temp_ref[0]
    target = jnp.zeros((tokens, LANES), jnp.int32)
    for i in range(tokens):
        target = jnp.where(row == i, tgt_ref[i], target)
    target = target - me * shard
    target = jnp.where(target < shard, target, -1)

    def softmax_step(carry, at, ts, store):
        m, s, tg = carry
        new_m = m
        for b, t in enumerate(ts):
            tg = tg + jnp.where(lane + (at + b * LANES) == target, t, 0.0)
            new_m = jnp.maximum(new_m, t)
        s = s * jnp.exp(m - new_m)
        for b, t in enumerate(ts):
            p = jnp.exp(t - new_m)
            s = s + p
            store(b, p)
        return new_m, s, tg

    def absorb(k, carry):
        def store(b, p):
            pexp_ref[k, :, b * LANES:(b + 1) * LANES] = p
        ts = [(mine[nch + k, :, b * LANES:(b + 1) * LANES] + rx[k, :, b * LANES:(b + 1) * LANES]) * factor
              for b in range(NBLK)]
        carry = softmax_step(carry, k * chunk, ts, store)
        peak_ref[k] = carry[0]
        return carry

    def absorb_tail(carry):
        pltpu.make_async_copy(tin, tin, trecv.at[0]).wait()

        def store(b, p):
            ptail_ref[:, b * LANES:(b + 1) * LANES] = p
        ts = []
        for b in range(TAIL):
            cols = slice(b * LANES, (b + 1) * LANES)
            t = ((tout[3, :, cols] + tin[2, :, cols]) + (tin[0, :, cols] + tin[1, :, cols])) * factor
            ts.append(jnp.where(lane + (tail_at + b * LANES) < shard, t, -jnp.inf))
        carry = softmax_step(carry, tail_at, ts, store)
        peak_ref[nch] = carry[0]
        return carry

    zeros = jnp.zeros((tokens, LANES), jnp.float32)
    carry = (zeros - jnp.inf, zeros, zeros)
    for j, end in enumerate(JOINT):
        begin = JOINT[j - 1] if j else 0
        first, count = starts[begin], sum(GROUPS[begin:end])
        arrived = rx.at[pl.ds(first, count)]
        pltpu.make_async_copy(arrived, arrived, xrecv.at[j]).wait()
        carry = lax.fori_loop(first, first + count, absorb, carry)
        if j == 0:
            carry = absorb_tail(carry)
    m, s, tg = carry

    def stat_send(i, peer):
        return pltpu.make_async_remote_copy(
            src_ref=stat_out, dst_ref=stat_in.at[i], send_sem=ssend.at[0], recv_sem=srecv.at[i],
            device_id={'tp': peer}, device_id_type=MESH)

    def merge(a, b):
        big = jnp.maximum(a[0], b[0])
        return big, a[1] * jnp.exp(a[0] - big) + b[1] * jnp.exp(b[0] - big), a[2] + b[2]

    field = LANES // 4

    def received(i):
        stat_send(i, partner).wait_recv()
        return [jnp.broadcast_to(stat_in[i, :, j * field:j * field + 1], (tokens, LANES)) for j in range(3)]

    def put(values):
        top, total, picked = values
        stat_out[...] = jnp.where(lane < field, top, jnp.where(lane < 2 * field, total, picked))

    def conclude(stats):
        big, total, picked = stats
        stat_ref[0] = big + jnp.log(total)
        stat_ref[1] = picked

    top = jnp.max(m, axis=-1, keepdims=True)
    total = jnp.sum(s * jnp.exp(m - top), axis=-1, keepdims=True)
    picked = jnp.sum(tg, axis=-1, keepdims=True)
    own_stat = [jnp.broadcast_to(v, (tokens, LANES)) for v in (top, total, picked)]

    @pl.when(core == FAR)
    def _():
        put(own_stat)
        stat_send(1, partner).start()
        chip_stat = received(1)
        conclude(merge(chip_stat, received(0)))
        stat_send(1, partner).wait_send()

    @pl.when(core != FAR)
    def _():
        chip_stat = merge(own_stat, received(1))
        put(chip_stat)
        stat_send(0, diag).start()
        stat_send(0, across).start()
        stat_send(1, partner).start()
        conclude(merge(chip_stat, received(0)))
        pltpu.make_async_copy(stat_all, stat_all, ssend.at[0]).wait()

    pltpu.make_async_copy(stg, stg, psend.at[0]).wait()
    pltpu.make_async_copy(rx, rx, xsend.at[0]).wait()
    pltpu.make_async_copy(tin, tin, tsend.at[0]).wait()


def finish_kernel(pexp_ref, ptail_ref, peak_ref, stat_ref, probs_hbm, ln_hbm, tl_hbm,
                  buf, ln_buf, tl_buf, sem, vec_sem):
    tokens = stat_ref.shape[1]
    nch, _, chunk = pexp_ref.shape
    shard = buf.shape[1]
    log_norm = stat_ref[0]
    picked = stat_ref[1]
    copies = []
    for j in range(PIECES):
        lo, hi = nch * j // PIECES, nch * (j + 1) // PIECES
        for k in range(lo, hi):
            scale = jnp.exp(peak_ref[k] - log_norm)
            for b in range(chunk // LANES):
                p = pexp_ref[k, :, b * LANES:(b + 1) * LANES] * scale
                buf[:, k * chunk + b * LANES:k * chunk + (b + 1) * LANES] = p.astype(jnp.bfloat16)
        end = hi * chunk
        if j == PIECES - 1:
            scale = jnp.exp(peak_ref[nch] - log_norm)
            for at in range(end, shard, LANES):
                p = (ptail_ref[:, at - end:at - end + LANES] * scale).astype(jnp.bfloat16)
                buf[:, at:min(at + LANES, shard)] = p[:, :min(LANES, shard - at)]
            end = shard
        cols = pl.ds(lo * chunk, end - lo * chunk)
        copies.append(pltpu.make_async_copy(buf.at[:, cols], probs_hbm.at[:, cols], sem.at[j]))
        copies[-1].start()
        if j == 1:
            lane = lax.broadcasted_iota(jnp.int32, (tokens, LANES), 1)
            row = lax.broadcasted_iota(jnp.int32, (tokens, LANES), 0)
            for i, (tmp, out, val) in enumerate(((ln_buf, ln_hbm, log_norm),
                                                 (tl_buf, tl_hbm, picked - log_norm))):
                tmp[...] = jnp.sum(jnp.where(row == lane, val, 0.0), axis=0)[:tokens]
                copies.append(pltpu.make_async_copy(tmp, out, vec_sem.at[i]))
                copies[-1].start()
    for copy in copies:
        copy.wait()


def solution(mesh):
    tp = mesh.shape['tp']

    def local_scores(hidden, final_gain, table_cols, targets, temperature):
        tokens, width = hidden.shape
        vocab, rows = table_cols.shape
        shard = vocab // tp
        chunk = NBLK * LANES
        nch = sum(GROUPS)
        f32, bf16 = jnp.float32, jnp.bfloat16

        def body(*refs):
            head_kernel(rows, vocab, tp, *refs)

        def in_hbm(a):
            return pltpu.with_memory_space_constraint(a, pltpu.HBM)

        def dma(n):
            return pltpu.SemaphoreType.DMA((n,))

        vm = pl.BlockSpec(memory_space=pltpu.VMEM)
        hbm = pl.BlockSpec(memory_space=pltpu.HBM)
        outs = pl.pallas_call(
            body,
            out_shape=(pltpu.VMEM((nch, tokens, chunk), f32),
                       pltpu.VMEM((tokens, TAIL * LANES), f32),
                       pltpu.VMEM((nch + 1, tokens, LANES), f32),
                       pltpu.VMEM((2, tokens, LANES), f32)),
            in_specs=[hbm, hbm, hbm, pl.BlockSpec(memory_space=pltpu.SMEM), hbm],
            out_specs=(vm, vm, vm, vm),
            scratch_shapes=[
                pltpu.VMEM((DEPTH * 2, rows, chunk + LANES), bf16),
                pltpu.VMEM((2, rows, (TAIL + 1) * LANES), bf16),
                pltpu.VMEM((2 * nch, tokens, chunk), f32),
                pltpu.VMEM((2 * nch, tokens, chunk), f32),
                pltpu.VMEM((2 * nch, tokens, chunk), f32),
                pltpu.VMEM((nch, tokens, chunk), f32),
                pltpu.VMEM((4, tokens, TAIL * LANES), f32),
                pltpu.VMEM((3, tokens, TAIL * LANES), f32),
                pltpu.VMEM((tokens, LANES), f32),
                pltpu.VMEM((2, tokens, LANES), f32),
                pltpu.VMEM((3, tokens, LANES), f32),
                pltpu.VMEM((tokens, rows), bf16),
                pltpu.VMEM((tokens, width), bf16),
                pltpu.VMEM((width // LANES, LANES), bf16),
                pltpu.SMEM((tokens,), jnp.int32),
                dma(3), dma(DEPTH * 2), dma(2), dma(1), dma(RING), dma(1), dma(len(JOINT)),
                dma(1), dma(1), dma(1), dma(2), pltpu.SemaphoreType.REGULAR,
            ],
            compiler_params=pltpu.CompilerParams(
                collective_id=0, has_side_effects=True, vmem_limit_bytes=40 * 1024 * 1024),
        )(in_hbm(hidden), in_hbm(final_gain.reshape(width // LANES, LANES)), in_hbm(targets),
          temperature.reshape(1), in_hbm(table_cols.T))
        probs, ln, tl = pl.pallas_call(
            finish_kernel,
            out_shape=(pltpu.HBM((tokens, shard), bf16), pltpu.HBM((tokens,), f32), pltpu.HBM((tokens,), f32)),
            in_specs=[vm, vm, vm, vm],
            out_specs=(hbm, hbm, hbm),
            scratch_shapes=[
                pltpu.VMEM((tokens, shard), bf16), pltpu.VMEM((tokens,), f32), pltpu.VMEM((tokens,), f32),
                dma(PIECES), dma(2),
            ],
            compiler_params=pltpu.CompilerParams(vmem_limit_bytes=8 * 1024 * 1024),
        )(*(pltpu.with_memory_space_constraint(a, pltpu.VMEM) for a in outs))
        return ln, tl, probs

    return jax.shard_map(local_scores, mesh=mesh,
                         in_specs=(P('dp', None), P(None), P(None, 'tp'), P('dp'), P()),
                         out_specs=(P('dp'), P('dp'), P('dp', 'tp')),
                         check_vma=False)
```

```python
import jax
import jax.numpy as jnp
from jax import lax
from jax.experimental import pallas as pl
from jax.experimental.pallas import tpu as pltpu
from jax.sharding import PartitionSpec as P

NORM_EPS = 1e-6
LANES = 128
NBLK = 7
TAIL = 3
DEPTH = 3
RING = 6
GROUPS = (1, 1, 2, 4, 6, 8, 8, 8, 3, 1)
FAR = 0
HELD = 5
HOLD = 36
JOINT = (8, 9, 10)
PIECES = 6
MESH = pl.DeviceIdType.MESH


def dot(u, window):
    return jnp.dot(u, window, preferred_element_type=jnp.float32)


def head_kernel(rows, vocab, tp,
                hid_hbm, gain_hbm, tgt_hbm, temp_ref, tab_ref,
                pexp_ref, ptail_ref, peak_ref, stat_ref,
                win, twin, stg, mine, part, rx, tout, tin, stat_out, stat_in, stat_all, ubuf,
                hid_ref, gain_ref, tgt_ref,
                in_sem, win_sem, twin_sem, psend, precv, xsend, xrecv, tsend, trecv, ssend, srecv, go):
    me = lax.axis_index('tp')
    chip = me // 2
    core = me % 2
    partner = chip * 2 + (1 - core)
    across = (1 - chip) * 2 + core
    diag = (1 - chip) * 2 + (1 - core)
    shard = vocab // tp
    tokens, width = hid_hbm.shape
    chunk = NBLK * LANES
    nch = sum(GROUPS)
    steps = 2 * nch
    tail_at = nch * chunk
    last_blk = vocab // LANES - 1

    barrier = pltpu.get_barrier_semaphore()
    for peer in (partner, diag):
        pl.semaphore_signal(barrier, inc=1, device_id={'tp': peer}, device_id_type=MESH)

    @pl.when(core != FAR)
    def _():
        pl.semaphore_signal(barrier, inc=1, device_id={'tp': across}, device_id_type=MESH)

    small = [pltpu.make_async_copy(src, dst, in_sem.at[i]) for i, (src, dst) in enumerate((
        (hid_hbm, hid_ref), (gain_hbm, gain_ref), (tgt_hbm, tgt_ref)))]

    def window(g, which):
        far = g < nch
        k = jnp.where(far, g, g - nch)
        there = jnp.where(far, 1 - chip, chip)
        dest = there * 2 + (jnp.where(which == 0, 1 - core, core))
        blk = (dest * shard) // LANES + k * NBLK
        slot = (g % DEPTH) * 2 + which
        return pltpu.make_async_copy(
            tab_ref.at[:, pl.ds(pl.multiple_of(blk * LANES, LANES), chunk + LANES)],
            win.at[slot], win_sem.at[slot]), dest, slot

    def fetch(g, which):
        window(g, which)[0].start()

    def tail_window(i, dest):
        blk = (dest * shard) // LANES + nch * NBLK
        edge = jnp.minimum(blk + TAIL, last_blk)
        for at, first, count in ((blk, 0, TAIL), (edge, TAIL, 1)):
            pltpu.make_async_copy(
                tab_ref.at[:, pl.ds(pl.multiple_of(at * LANES, LANES), count * LANES)],
                twin.at[i % 2, :, pl.ds(first * LANES, count * LANES)], twin_sem.at[i % 2]).start()

    tail_dests = ((1 - chip) * 2 + (1 - FAR), (1 - chip) * 2 + FAR, partner, me)
    small[0].start()
    small[1].start()
    fetch(0, 0)
    tail_window(0, tail_dests[0])
    tail_window(1, tail_dests[1])
    fetch(0, 1)
    small[0].wait()
    small[1].wait()

    x = hid_ref[...].astype(jnp.float32)
    inv_rms = lax.rsqrt(jnp.mean(x * x, axis=-1, keepdims=True) + NORM_EPS)
    gain = jnp.concatenate([gain_ref[i:i + 1] for i in range(width // LANES)], axis=1).astype(jnp.float32)
    own, own_gain = x[:, :rows], gain[:, :rows]
    for t in range(1, tp):
        cols = slice(t * rows, (t + 1) * rows)
        own = jnp.where(me == t, x[:, cols], own)
        own_gain = jnp.where(me == t, gain[:, cols], own_gain)
    ubuf[...] = (own * inv_rms * own_gain).astype(jnp.bfloat16)

    lane = lax.broadcasted_iota(jnp.int32, (tokens, LANES), 1)
    row = lax.broadcasted_iota(jnp.int32, (tokens, LANES), 0)

    def place(z, dest, blocks, store):
        back = LANES - (dest * shard) % LANES
        rolled = [pltpu.roll(z[:, b * LANES:(b + 1) * LANES], back, 1) for b in range(blocks + 1)]
        for b in range(blocks):
            store(b, jnp.where(lane < back, rolled[b], rolled[b + 1]))

    def tail_logits(i):
        pltpu.make_async_copy(tab_ref.at[:, pl.ds(0, (TAIL + 1) * LANES)], twin.at[i % 2], twin_sem.at[i % 2]).wait()

        def store(b, v):
            tout[i, :, b * LANES:(b + 1) * LANES] = v
        place(dot(ubuf[...], twin[i % 2]), tail_dests[i], TAIL, store)

    def tail_send(i):
        slot = 2 if i == 2 else (jnp.where(core == FAR, 1 - i, i))
        return pltpu.make_async_remote_copy(
            src_ref=tout.at[i], dst_ref=tin.at[slot], send_sem=tsend.at[0], recv_sem=trecv.at[0],
            device_id={'tp': tail_dests[i]}, device_id_type=MESH)

    def to_partner(g):
        return pltpu.make_async_remote_copy(
            src_ref=stg.at[g], dst_ref=part.at[g], send_sem=psend.at[0], recv_sem=precv.at[g % RING],
            device_id={'tp': partner}, device_id_type=MESH)

    starts = [sum(GROUPS[:i]) for i in range(len(GROUPS))]

    def owner(i):
        return sum(i >= end for end in JOINT[:-1])

    def to_across(i):
        chunks = pl.ds(starts[i], GROUPS[i])
        return pltpu.make_async_remote_copy(
            src_ref=mine.at[chunks], dst_ref=rx.at[chunks], send_sem=xsend.at[0], recv_sem=xrecv.at[owner(i)],
            device_id={'tp': across}, device_id_type=MESH)

    def partial_logits(g, which, out):
        copy, dest, slot = window(g, which)
        copy.wait()

        def store(b, v):
            out[g, :, b * LANES:(b + 1) * LANES] = v
        place(dot(ubuf[...], win[slot]), dest, NBLK, store)

    def combine(g):
        to_partner(g).wait_recv()
        mine[g] = mine[g] + part[g]

    def fetch_next(g, which):
        @pl.when(g + DEPTH < steps)
        def _():
            fetch(g + DEPTH, which)

    def hand_over(g):
        partial_logits(g, 0, stg)
        to_partner(g).start()
        fetch_next(g, 0)

    def keep(g):
        partial_logits(g, 1, mine)
        fetch_next(g, 1)

    partial_logits(0, 0, stg)
    fetch(1, 0)
    fetch(1, 1)
    fetch(2, 0)
    fetch(2, 1)
    small[2].start()
    tail_logits(0)

    @pl.when(core == FAR)
    def _():
        pl.semaphore_wait(barrier, 2)

    @pl.when(core != FAR)
    def _():
        pl.semaphore_wait(barrier, 3)
        pl.semaphore_signal(go, inc=1, device_id={'tp': partner}, device_id_type=MESH)

    to_partner(0).start()
    tail_send(0).start()
    tail_logits(1)

    @pl.when(core == FAR)
    def _():
        pl.semaphore_wait(go, 1)

    tail_send(1).start()
    fetch(DEPTH, 0)
    hand_over(1)
    keep(0)
    combine(0)
    to_across(0).start()
    hand_over(2)
    keep(1)
    combine(1)
    to_across(1).start()
    tail_window(2, partner)
    tail_window(3, me)

    def step(g, _):
        @pl.when(g + 1 < steps)
        def _():
            hand_over(g + 1)
        keep(g)
        h = g - 1

        @pl.when(h >= 2)
        def _():
            combine(h)

        for i, first in enumerate(starts[2:], 2):
            ready = first + GROUPS[i] - 1

            @pl.when(h == jnp.where(core == FAR, ready, ready if i < HELD else max(ready, HOLD)))
            def _():
                to_across(i).start()
        return 0

    lax.fori_loop(2, steps, step, 0)
    tail_logits(2)
    tail_send(2).start()
    tail_logits(3)
    combine(steps - 1)

    small[2].wait()
    factor = 1.0 / temp_ref[0]
    target = jnp.zeros((tokens, LANES), jnp.int32)
    for i in range(tokens):
        target = jnp.where(row == i, tgt_ref[i], target)
    target = target - me * shard
    target = jnp.where(target < shard, target, -1)

    def softmax_step(carry, at, ts, store):
        m, s, tg = carry
        new_m = m
        for b, t in enumerate(ts):
            tg = tg + jnp.where(lane + (at + b * LANES) == target, t, 0.0)
            new_m = jnp.maximum(new_m, t)
        s = s * jnp.exp(m - new_m)
        for b, t in enumerate(ts):
            p = jnp.exp(t - new_m)
            s = s + p
            store(b, p)
        return new_m, s, tg

    def absorb(k, carry):
        def store(b, p):
            pexp_ref[k, :, b * LANES:(b + 1) * LANES] = p
        ts = [(mine[nch + k, :, b * LANES:(b + 1) * LANES] + rx[k, :, b * LANES:(b + 1) * LANES]) * factor
              for b in range(NBLK)]
        carry = softmax_step(carry, k * chunk, ts, store)
        peak_ref[k] = carry[0]
        return carry

    def absorb_tail(carry):
        pltpu.make_async_copy(tin, tin, trecv.at[0]).wait()

        def store(b, p):
            ptail_ref[:, b * LANES:(b + 1) * LANES] = p
        ts = []
        for b in range(TAIL):
            cols = slice(b * LANES, (b + 1) * LANES)
            t = ((tout[3, :, cols] + tin[2, :, cols]) + (tin[0, :, cols] + tin[1, :, cols])) * factor
            ts.append(jnp.where(lane + (tail_at + b * LANES) < shard, t, -jnp.inf))
        carry = softmax_step(carry, tail_at, ts, store)
        peak_ref[nch] = carry[0]
        return carry

    def stat_send(i, peer):
        return pltpu.make_async_remote_copy(
            src_ref=stat_out, dst_ref=stat_in.at[i], send_sem=ssend.at[0], recv_sem=srecv.at[i],
            device_id={'tp': peer}, device_id_type=MESH)

    def merge(a, b):
        big = jnp.maximum(a[0], b[0])
        return big, a[1] * jnp.exp(a[0] - big) + b[1] * jnp.exp(b[0] - big), a[2] + b[2]

    field = LANES // 4

    def received(i):
        stat_send(i, partner).wait_recv()
        return [jnp.broadcast_to(stat_in[i, :, j * field:j * field + 1], (tokens, LANES)) for j in range(3)]

    def put(values):
        top, total, picked = values
        stat_out[...] = jnp.where(lane < field, top, jnp.where(lane < 2 * field, total, picked))

    def conclude(stats):
        big, total, picked = stats
        stat_ref[0] = big + jnp.log(total)
        stat_ref[1] = picked

    def take_partner(carry):
        big, total, picked = merge(carry, received(1))
        only = lane == 0
        alone = carry[1] * jnp.exp(carry[0] - big)
        return big, jnp.where(only, total, alone), jnp.where(only, picked, carry[2])

    zeros = jnp.zeros((tokens, LANES), jnp.float32)
    carry = (zeros - jnp.inf, zeros, zeros)
    for j, end in enumerate(JOINT):
        begin = JOINT[j - 1] if j else 0
        if j == len(JOINT) - 1:
            carry = lax.cond(core == FAR, lambda c: c, take_partner, carry)
        first, count = starts[begin], sum(GROUPS[begin:end])
        arrived = rx.at[pl.ds(first, count)]
        pltpu.make_async_copy(arrived, arrived, xrecv.at[j]).wait()
        carry = lax.fori_loop(first, first + count, absorb, carry)
        if j == 0:
            carry = absorb_tail(carry)
    m, s, tg = carry

    top = jnp.max(m, axis=-1, keepdims=True)
    total = jnp.sum(s * jnp.exp(m - top), axis=-1, keepdims=True)
    picked = jnp.sum(tg, axis=-1, keepdims=True)
    own_stat = [jnp.broadcast_to(v, (tokens, LANES)) for v in (top, total, picked)]

    @pl.when(core == FAR)
    def _():
        put(own_stat)
        stat_send(1, partner).start()
        chip_stat = received(1)
        conclude(merge(chip_stat, received(0)))
        stat_send(1, partner).wait_send()

    @pl.when(core != FAR)
    def _():
        chip_stat = own_stat
        put(chip_stat)
        stat_send(0, diag).start()
        stat_send(0, across).start()
        stat_send(1, partner).start()
        conclude(merge(chip_stat, received(0)))
        pltpu.make_async_copy(stat_all, stat_all, ssend.at[0]).wait()

    pltpu.make_async_copy(stg, stg, psend.at[0]).wait()
    pltpu.make_async_copy(rx, rx, xsend.at[0]).wait()
    pltpu.make_async_copy(tin, tin, tsend.at[0]).wait()


def finish_kernel(pexp_ref, ptail_ref, peak_ref, stat_ref, probs_hbm, ln_hbm, tl_hbm,
                  buf, ln_buf, tl_buf, sem, vec_sem):
    tokens = stat_ref.shape[1]
    nch, _, chunk = pexp_ref.shape
    shard = buf.shape[1]
    log_norm = stat_ref[0]
    picked = stat_ref[1]
    copies = []
    for j in range(PIECES):
        lo, hi = nch * j // PIECES, nch * (j + 1) // PIECES
        for k in range(lo, hi):
            scale = jnp.exp(peak_ref[k] - log_norm)
            for b in range(chunk // LANES):
                p = pexp_ref[k, :, b * LANES:(b + 1) * LANES] * scale
                buf[:, k * chunk + b * LANES:k * chunk + (b + 1) * LANES] = p.astype(jnp.bfloat16)
        end = hi * chunk
        if j == PIECES - 1:
            scale = jnp.exp(peak_ref[nch] - log_norm)
            for at in range(end, shard, LANES):
                p = (ptail_ref[:, at - end:at - end + LANES] * scale).astype(jnp.bfloat16)
                buf[:, at:min(at + LANES, shard)] = p[:, :min(LANES, shard - at)]
            end = shard
        cols = pl.ds(lo * chunk, end - lo * chunk)
        copies.append(pltpu.make_async_copy(buf.at[:, cols], probs_hbm.at[:, cols], sem.at[j]))
        copies[-1].start()
        if j == 1:
            lane = lax.broadcasted_iota(jnp.int32, (tokens, LANES), 1)
            row = lax.broadcasted_iota(jnp.int32, (tokens, LANES), 0)
            for i, (tmp, out, val) in enumerate(((ln_buf, ln_hbm, log_norm),
                                                 (tl_buf, tl_hbm, picked - log_norm))):
                tmp[...] = jnp.sum(jnp.where(row == lane, val, 0.0), axis=0)[:tokens]
                copies.append(pltpu.make_async_copy(tmp, out, vec_sem.at[i]))
                copies[-1].start()
    for copy in copies:
        copy.wait()


def solution(mesh):
    tp = mesh.shape['tp']

    def local_scores(hidden, final_gain, table_cols, targets, temperature):
        tokens, width = hidden.shape
        vocab, rows = table_cols.shape
        shard = vocab // tp
        chunk = NBLK * LANES
        nch = sum(GROUPS)
        f32, bf16 = jnp.float32, jnp.bfloat16

        def body(*refs):
            head_kernel(rows, vocab, tp, *refs)

        def in_hbm(a):
            return pltpu.with_memory_space_constraint(a, pltpu.HBM)

        def dma(n):
            return pltpu.SemaphoreType.DMA((n,))

        vm = pl.BlockSpec(memory_space=pltpu.VMEM)
        hbm = pl.BlockSpec(memory_space=pltpu.HBM)
        outs = pl.pallas_call(
            body,
            out_shape=(pltpu.VMEM((nch, tokens, chunk), f32),
                       pltpu.VMEM((tokens, TAIL * LANES), f32),
                       pltpu.VMEM((nch + 1, tokens, LANES), f32),
                       pltpu.VMEM((2, tokens, LANES), f32)),
            in_specs=[hbm, hbm, hbm, pl.BlockSpec(memory_space=pltpu.SMEM), hbm],
            out_specs=(vm, vm, vm, vm),
            scratch_shapes=[
                pltpu.VMEM((DEPTH * 2, rows, chunk + LANES), bf16),
                pltpu.VMEM((2, rows, (TAIL + 1) * LANES), bf16),
                pltpu.VMEM((2 * nch, tokens, chunk), f32),
                pltpu.VMEM((2 * nch, tokens, chunk), f32),
                pltpu.VMEM((2 * nch, tokens, chunk), f32),
                pltpu.VMEM((nch, tokens, chunk), f32),
                pltpu.VMEM((4, tokens, TAIL * LANES), f32),
                pltpu.VMEM((3, tokens, TAIL * LANES), f32),
                pltpu.VMEM((tokens, LANES), f32),
                pltpu.VMEM((2, tokens, LANES), f32),
                pltpu.VMEM((3, tokens, LANES), f32),
                pltpu.VMEM((tokens, rows), bf16),
                pltpu.VMEM((tokens, width), bf16),
                pltpu.VMEM((width // LANES, LANES), bf16),
                pltpu.SMEM((tokens,), jnp.int32),
                dma(3), dma(DEPTH * 2), dma(2), dma(1), dma(RING), dma(1), dma(len(JOINT)),
                dma(1), dma(1), dma(1), dma(2), pltpu.SemaphoreType.REGULAR,
            ],
            compiler_params=pltpu.CompilerParams(
                collective_id=0, has_side_effects=True, vmem_limit_bytes=40 * 1024 * 1024),
        )(in_hbm(hidden), in_hbm(final_gain.reshape(width // LANES, LANES)), in_hbm(targets),
          temperature.reshape(1), in_hbm(table_cols.T))
        probs, ln, tl = pl.pallas_call(
            finish_kernel,
            out_shape=(pltpu.HBM((tokens, shard), bf16), pltpu.HBM((tokens,), f32), pltpu.HBM((tokens,), f32)),
            in_specs=[vm, vm, vm, vm],
            out_specs=(hbm, hbm, hbm),
            scratch_shapes=[
                pltpu.VMEM((tokens, shard), bf16), pltpu.VMEM((tokens,), f32), pltpu.VMEM((tokens,), f32),
                dma(PIECES), dma(2),
            ],
            compiler_params=pltpu.CompilerParams(vmem_limit_bytes=8 * 1024 * 1024),
        )(*(pltpu.with_memory_space_constraint(a, pltpu.VMEM) for a in outs))
        return ln, tl, probs

    return jax.shard_map(local_scores, mesh=mesh,
                         in_specs=(P('dp', None), P(None), P(None, 'tp'), P('dp'), P()),
                         out_specs=(P('dp'), P('dp'), P('dp', 'tp')),
                         check_vma=False)
```

```python
import jax
import jax.numpy as jnp
from jax import lax
from jax.experimental import pallas as pl
from jax.experimental.pallas import tpu as pltpu
from jax.sharding import PartitionSpec as P

NORM_EPS = 1e-6
LANES = 128
NBLK = 7
TAIL = 3
DEPTH = 3
RING = 6
GROUPS = (1, 1, 2, 4, 6, 8, 8, 11, 1)
FAR = 0
HELD = 5
HOLD = 36
JOINT = (7, 8, 9)
PIECES = 6
MESH = pl.DeviceIdType.MESH


def dot(u, window):
    return jnp.dot(u, window, preferred_element_type=jnp.float32)


def head_kernel(rows, vocab, tp,
                hid_hbm, gain_hbm, tgt_hbm, temp_ref, tab_ref,
                pexp_ref, ptail_ref, peak_ref, stat_ref,
                win, twin, stg, mine, part, rx, tout, tin, stat_out, stat_in, stat_all, ubuf,
                hid_ref, gain_ref, tgt_ref,
                in_sem, win_sem, twin_sem, psend, precv, xsend, xrecv, tsend, trecv, ssend, srecv, go):
    me = lax.axis_index('tp')
    chip = me // 2
    core = me % 2
    partner = chip * 2 + (1 - core)
    across = (1 - chip) * 2 + core
    diag = (1 - chip) * 2 + (1 - core)
    shard = vocab // tp
    tokens, width = hid_hbm.shape
    chunk = NBLK * LANES
    nch = sum(GROUPS)
    steps = 2 * nch
    tail_at = nch * chunk
    last_blk = vocab // LANES - 1

    barrier = pltpu.get_barrier_semaphore()
    for peer in (partner, diag):
        pl.semaphore_signal(barrier, inc=1, device_id={'tp': peer}, device_id_type=MESH)

    @pl.when(core != FAR)
    def _():
        pl.semaphore_signal(barrier, inc=1, device_id={'tp': across}, device_id_type=MESH)

    small = [pltpu.make_async_copy(src, dst, in_sem.at[i % 2]) for i, (src, dst) in enumerate((
        (hid_hbm, hid_ref), (gain_hbm, gain_ref), (tgt_hbm, tgt_ref)))]

    def window(g, which):
        far = g < nch
        k = jnp.where(far, g, g - nch)
        there = jnp.where(far, 1 - chip, chip)
        dest = there * 2 + (jnp.where(which == 0, 1 - core, core))
        blk = (dest * shard) // LANES + k * NBLK
        slot = (g % DEPTH) * 2 + which
        return pltpu.make_async_copy(
            tab_ref.at[:, pl.ds(pl.multiple_of(blk * LANES, LANES), chunk + LANES)],
            win.at[slot], win_sem.at[slot]), dest, slot

    def fetch(g, which):
        window(g, which)[0].start()

    def tail_window(i, dest):
        blk = (dest * shard) // LANES + nch * NBLK
        edge = jnp.minimum(blk + TAIL, last_blk)
        for at, first, count in ((blk, 0, TAIL), (edge, TAIL, 1)):
            pltpu.make_async_copy(
                tab_ref.at[:, pl.ds(pl.multiple_of(at * LANES, LANES), count * LANES)],
                twin.at[i % 2, :, pl.ds(first * LANES, count * LANES)], twin_sem.at[i % 2]).start()

    tail_dests = ((1 - chip) * 2 + (1 - FAR), (1 - chip) * 2 + FAR, partner, me)
    small[0].start()
    small[1].start()
    fetch(0, 0)
    tail_window(0, tail_dests[0])
    tail_window(1, tail_dests[1])
    fetch(0, 1)
    small[0].wait()
    small[1].wait()

    x = hid_ref[...].astype(jnp.float32)
    inv_rms = lax.rsqrt(jnp.mean(x * x, axis=-1, keepdims=True) + NORM_EPS)
    gain = jnp.concatenate([gain_ref[i:i + 1] for i in range(width // LANES)], axis=1).astype(jnp.float32)
    own, own_gain = x[:, :rows], gain[:, :rows]
    for t in range(1, tp):
        cols = slice(t * rows, (t + 1) * rows)
        own = jnp.where(me == t, x[:, cols], own)
        own_gain = jnp.where(me == t, gain[:, cols], own_gain)
    ubuf[...] = (own * inv_rms * own_gain).astype(jnp.bfloat16)

    lane = lax.broadcasted_iota(jnp.int32, (tokens, LANES), 1)
    row = lax.broadcasted_iota(jnp.int32, (tokens, LANES), 0)

    def place(z, dest, blocks, store):
        back = LANES - (dest * shard) % LANES
        rolled = [pltpu.roll(z[:, b * LANES:(b + 1) * LANES], back, 1) for b in range(blocks + 1)]
        for b in range(blocks):
            store(b, jnp.where(lane < back, rolled[b], rolled[b + 1]))

    def tail_logits(i):
        pltpu.make_async_copy(tab_ref.at[:, pl.ds(0, (TAIL + 1) * LANES)], twin.at[i % 2], twin_sem.at[i % 2]).wait()

        def store(b, v):
            tout[i, :, b * LANES:(b + 1) * LANES] = v
        place(dot(ubuf[...], twin[i % 2]), tail_dests[i], TAIL, store)

    def tail_send(i):
        slot = 2 if i == 2 else (jnp.where(core == FAR, 1 - i, i))
        return pltpu.make_async_remote_copy(
            src_ref=tout.at[i], dst_ref=tin.at[slot], send_sem=tsend.at[0], recv_sem=trecv.at[0],
            device_id={'tp': tail_dests[i]}, device_id_type=MESH)

    def to_partner(g):
        return pltpu.make_async_remote_copy(
            src_ref=stg.at[g], dst_ref=part.at[g], send_sem=psend.at[0], recv_sem=precv.at[g % RING],
            device_id={'tp': partner}, device_id_type=MESH)

    starts = [sum(GROUPS[:i]) for i in range(len(GROUPS))]

    def owner(i):
        return sum(i >= end for end in JOINT[:-1])

    def to_across(i):
        chunks = pl.ds(starts[i], GROUPS[i])
        return pltpu.make_async_remote_copy(
            src_ref=mine.at[chunks], dst_ref=rx.at[chunks], send_sem=xsend.at[0], recv_sem=xrecv.at[owner(i)],
            device_id={'tp': across}, device_id_type=MESH)

    def partial_logits(g, which, out):
        copy, dest, slot = window(g, which)
        copy.wait()

        def store(b, v):
            out[g, :, b * LANES:(b + 1) * LANES] = v
        place(dot(ubuf[...], win[slot]), dest, NBLK, store)

    def combine(g):
        to_partner(g).wait_recv()
        mine[g] = mine[g] + part[g]

    def fetch_next(g, which):
        @pl.when(g + DEPTH < steps)
        def _():
            fetch(g + DEPTH, which)

    def hand_over(g):
        partial_logits(g, 0, stg)
        to_partner(g).start()
        fetch_next(g, 0)

    def keep(g):
        partial_logits(g, 1, mine)
        fetch_next(g, 1)

    partial_logits(0, 0, stg)
    fetch(1, 0)
    fetch(1, 1)
    fetch(2, 0)
    fetch(2, 1)
    small[2].start()
    tail_logits(0)

    @pl.when(core == FAR)
    def _():
        pl.semaphore_wait(barrier, 2)

    @pl.when(core != FAR)
    def _():
        pl.semaphore_wait(barrier, 3)
        pl.semaphore_signal(go, inc=1, device_id={'tp': partner}, device_id_type=MESH)

    to_partner(0).start()
    tail_send(0).start()
    tail_logits(1)

    @pl.when(core == FAR)
    def _():
        pl.semaphore_wait(go, 1)

    tail_send(1).start()
    fetch(DEPTH, 0)
    hand_over(1)
    keep(0)
    combine(0)
    to_across(0).start()
    hand_over(2)
    keep(1)
    combine(1)
    to_across(1).start()
    tail_window(2, partner)
    tail_window(3, me)

    def step(g, _):
        @pl.when(g + 1 < steps)
        def _():
            hand_over(g + 1)
        keep(g)
        h = g - 1

        @pl.when(h >= 2)
        def _():
            combine(h)

        for i, first in enumerate(starts[2:], 2):
            ready = first + GROUPS[i] - 1

            @pl.when(h == jnp.where(core == FAR, ready, ready if i < HELD else max(ready, HOLD)))
            def _():
                to_across(i).start()
        return 0

    lax.fori_loop(2, steps, step, 0)
    tail_logits(2)
    tail_send(2).start()
    tail_logits(3)
    combine(steps - 1)

    small[2].wait()
    factor = 1.0 / temp_ref[0]
    target = jnp.zeros((tokens, LANES), jnp.int32)
    for i in range(tokens):
        target = jnp.where(row == i, tgt_ref[i], target)
    target = target - me * shard
    target = jnp.where(target < shard, target, -1)

    def softmax_step(carry, at, ts, store):
        m, s, tg = carry
        new_m = m
        for b, t in enumerate(ts):
            tg = tg + jnp.where(lane + (at + b * LANES) == target, t, 0.0)
            new_m = jnp.maximum(new_m, t)
        s = s * jnp.exp(m - new_m)
        for b, t in enumerate(ts):
            p = jnp.exp(t - new_m)
            s = s + p
            store(b, p)
        return new_m, s, tg

    def absorb(k, carry):
        def store(b, p):
            pexp_ref[k, :, b * LANES:(b + 1) * LANES] = p
        ts = [(mine[nch + k, :, b * LANES:(b + 1) * LANES] + rx[k, :, b * LANES:(b + 1) * LANES]) * factor
              for b in range(NBLK)]
        carry = softmax_step(carry, k * chunk, ts, store)
        peak_ref[k] = carry[0]
        return carry

    def absorb_tail(carry):
        pltpu.make_async_copy(tin, tin, trecv.at[0]).wait()

        def store(b, p):
            ptail_ref[:, b * LANES:(b + 1) * LANES] = p
        ts = []
        for b in range(TAIL):
            cols = slice(b * LANES, (b + 1) * LANES)
            t = ((tout[3, :, cols] + tin[2, :, cols]) + (tin[0, :, cols] + tin[1, :, cols])) * factor
            ts.append(jnp.where(lane + (tail_at + b * LANES) < shard, t, -jnp.inf))
        carry = softmax_step(carry, tail_at, ts, store)
        peak_ref[nch] = carry[0]
        return carry

    def stat_send(i, peer):
        return pltpu.make_async_remote_copy(
            src_ref=stat_out, dst_ref=stat_in.at[i], send_sem=ssend.at[0], recv_sem=srecv.at[i],
            device_id={'tp': peer}, device_id_type=MESH)

    def merge(a, b):
        big = jnp.maximum(a[0], b[0])
        return big, a[1] * jnp.exp(a[0] - big) + b[1] * jnp.exp(b[0] - big), a[2] + b[2]

    field = LANES // 8
    half = tokens // 2

    def received(i):
        stat_send(i, partner).wait_recv()
        columns = [stat_in[i, :, j * field:j * field + 1] for j in range(6)]
        wide = [jnp.broadcast_to(c, (half, LANES)) for c in columns]
        return [jnp.concatenate(wide[2 * j:2 * j + 2], axis=0) for j in range(3)]

    def put(values):
        tile = values[2][half:]
        fields = [v[lo:lo + half] for v in values for lo in (0, half)]
        for j in range(4, -1, -1):
            tile = jnp.where(lane[:half] < (j + 1) * field, fields[j], tile)
        stat_out[...] = tile

    def conclude(stats):
        big, total, picked = stats
        stat_ref[0] = big + jnp.log(total)
        stat_ref[1] = picked

    def take_partner(carry):
        big, total, picked = merge(carry, received(1))
        only = lane == 0
        alone = carry[1] * jnp.exp(carry[0] - big)
        return big, jnp.where(only, total, alone), jnp.where(only, picked, carry[2])

    zeros = jnp.zeros((tokens, LANES), jnp.float32)
    carry = (zeros - jnp.inf, zeros, zeros)
    for j, end in enumerate(JOINT):
        begin = JOINT[j - 1] if j else 0
        if j == len(JOINT) - 1:
            carry = lax.cond(core == FAR, lambda c: c, take_partner, carry)
        first, count = starts[begin], sum(GROUPS[begin:end])
        arrived = rx.at[pl.ds(first, count)]
        pltpu.make_async_copy(arrived, arrived, xrecv.at[j]).wait()
        carry = lax.fori_loop(first, first + count, absorb, carry)
        if j == 0:
            carry = absorb_tail(carry)
    m, s, tg = carry

    top = jnp.max(m, axis=-1, keepdims=True)
    total = jnp.sum(s * jnp.exp(m - top), axis=-1, keepdims=True)
    picked = jnp.sum(tg, axis=-1, keepdims=True)
    own_stat = [jnp.broadcast_to(v, (tokens, LANES)) for v in (top, total, picked)]

    @pl.when(core == FAR)
    def _():
        put(own_stat)
        stat_send(1, partner).start()
        chip_stat = received(1)
        conclude(merge(chip_stat, received(0)))
        stat_send(1, partner).wait_send()

    @pl.when(core != FAR)
    def _():
        chip_stat = own_stat
        put(chip_stat)
        stat_send(0, diag).start()
        stat_send(0, across).start()
        stat_send(1, partner).start()
        conclude(merge(chip_stat, received(0)))
        pltpu.make_async_copy(stat_all, stat_all, ssend.at[0]).wait()

    pltpu.make_async_copy(stg, stg, psend.at[0]).wait()
    pltpu.make_async_copy(rx, rx, xsend.at[0]).wait()
    pltpu.make_async_copy(tin, tin, tsend.at[0]).wait()


def finish_kernel(pexp_ref, ptail_ref, peak_ref, stat_ref, probs_hbm, ln_hbm, tl_hbm,
                  buf, ln_buf, tl_buf, sem, vec_sem):
    tokens = stat_ref.shape[1]
    nch, _, chunk = pexp_ref.shape
    shard = buf.shape[1]
    log_norm = stat_ref[0]
    picked = stat_ref[1]
    copies = []
    for j in range(PIECES):
        lo, hi = nch * j // PIECES, nch * (j + 1) // PIECES
        for k in range(lo, hi):
            scale = jnp.exp(peak_ref[k] - log_norm)
            for b in range(chunk // LANES):
                p = pexp_ref[k, :, b * LANES:(b + 1) * LANES] * scale
                buf[:, k * chunk + b * LANES:k * chunk + (b + 1) * LANES] = p.astype(jnp.bfloat16)
        end = hi * chunk
        if j == PIECES - 1:
            scale = jnp.exp(peak_ref[nch] - log_norm)
            for at in range(end, shard, LANES):
                p = (ptail_ref[:, at - end:at - end + LANES] * scale).astype(jnp.bfloat16)
                buf[:, at:min(at + LANES, shard)] = p[:, :min(LANES, shard - at)]
            end = shard
        cols = pl.ds(lo * chunk, end - lo * chunk)
        copies.append(pltpu.make_async_copy(buf.at[:, cols], probs_hbm.at[:, cols], sem.at[j]))
        copies[-1].start()
        if j == 1:
            lane = lax.broadcasted_iota(jnp.int32, (tokens, LANES), 1)
            row = lax.broadcasted_iota(jnp.int32, (tokens, LANES), 0)
            for i, (tmp, out, val) in enumerate(((ln_buf, ln_hbm, log_norm),
                                                 (tl_buf, tl_hbm, picked - log_norm))):
                tmp[...] = jnp.sum(jnp.where(row == lane, val, 0.0), axis=0)[:tokens]
                copies.append(pltpu.make_async_copy(tmp, out, vec_sem.at[i]))
                copies[-1].start()
    for copy in copies:
        copy.wait()


def solution(mesh):
    tp = mesh.shape['tp']

    def local_scores(hidden, final_gain, table_cols, targets, temperature):
        tokens, width = hidden.shape
        vocab, rows = table_cols.shape
        shard = vocab // tp
        chunk = NBLK * LANES
        nch = sum(GROUPS)
        f32, bf16 = jnp.float32, jnp.bfloat16

        def body(*refs):
            head_kernel(rows, vocab, tp, *refs)

        def in_hbm(a):
            return pltpu.with_memory_space_constraint(a, pltpu.HBM)

        def dma(n):
            return pltpu.SemaphoreType.DMA((n,))

        vm = pl.BlockSpec(memory_space=pltpu.VMEM)
        hbm = pl.BlockSpec(memory_space=pltpu.HBM)
        outs = pl.pallas_call(
            body,
            out_shape=(pltpu.VMEM((nch, tokens, chunk), f32),
                       pltpu.VMEM((tokens, TAIL * LANES), f32),
                       pltpu.VMEM((nch + 1, tokens, LANES), f32),
                       pltpu.VMEM((2, tokens, LANES), f32)),
            in_specs=[hbm, hbm, hbm, pl.BlockSpec(memory_space=pltpu.SMEM), hbm],
            out_specs=(vm, vm, vm, vm),
            scratch_shapes=[
                pltpu.VMEM((DEPTH * 2, rows, chunk + LANES), bf16),
                pltpu.VMEM((2, rows, (TAIL + 1) * LANES), bf16),
                pltpu.VMEM((2 * nch, tokens, chunk), f32),
                pltpu.VMEM((2 * nch, tokens, chunk), f32),
                pltpu.VMEM((2 * nch, tokens, chunk), f32),
                pltpu.VMEM((nch, tokens, chunk), f32),
                pltpu.VMEM((4, tokens, TAIL * LANES), f32),
                pltpu.VMEM((3, tokens, TAIL * LANES), f32),
                pltpu.VMEM((tokens // 2, LANES), f32),
                pltpu.VMEM((2, tokens // 2, LANES), f32),
                pltpu.VMEM((3, tokens // 2, LANES), f32),
                pltpu.VMEM((tokens, rows), bf16),
                pltpu.VMEM((tokens, width), bf16),
                pltpu.VMEM((width // LANES, LANES), bf16),
                pltpu.SMEM((tokens,), jnp.int32),
                dma(2), dma(DEPTH * 2), dma(2), dma(1), dma(RING), dma(1), dma(len(JOINT)),
                dma(1), dma(1), dma(1), dma(2), pltpu.SemaphoreType.REGULAR,
            ],
            compiler_params=pltpu.CompilerParams(
                collective_id=0, has_side_effects=True, vmem_limit_bytes=40 * 1024 * 1024),
        )(in_hbm(hidden), in_hbm(final_gain.reshape(width // LANES, LANES)), in_hbm(targets),
          temperature.reshape(1), in_hbm(table_cols.T))
        probs, ln, tl = pl.pallas_call(
            finish_kernel,
            out_shape=(pltpu.HBM((tokens, shard), bf16), pltpu.HBM((tokens,), f32), pltpu.HBM((tokens,), f32)),
            in_specs=[vm, vm, vm, vm],
            out_specs=(hbm, hbm, hbm),
            scratch_shapes=[
                pltpu.VMEM((tokens, shard), bf16), pltpu.VMEM((tokens,), f32), pltpu.VMEM((tokens,), f32),
                dma(PIECES), dma(2),
            ],
            compiler_params=pltpu.CompilerParams(vmem_limit_bytes=8 * 1024 * 1024),
        )(*(pltpu.with_memory_space_constraint(a, pltpu.VMEM) for a in outs))
        return ln, tl, probs

    return jax.shard_map(local_scores, mesh=mesh,
                         in_specs=(P('dp', None), P(None), P(None, 'tp'), P('dp'), P()),
                         out_specs=(P('dp'), P('dp'), P('dp', 'tp')),
                         check_vma=False)
```

```python
import jax
import jax.numpy as jnp
from jax import lax
from jax.experimental import pallas as pl
from jax.experimental.pallas import tpu as pltpu
from jax.sharding import PartitionSpec as P

NORM_EPS = 1e-6
LANES = 128
NBLK = 7
TAIL = 3
DEPTH = 3
RING = 6
GROUPS = (1, 1, 2, 4, 6, 8, 8, 11, 1)
FAR = 0
HELD = 5
HOLD = 36
JOINT = (7, 8, 9)
PIECES = (0, 2, 12, 22, 32, 42)
MESH = pl.DeviceIdType.MESH


def dot(u, window):
    return jnp.dot(u, window, preferred_element_type=jnp.float32)


def head_kernel(rows, vocab, tp,
                hid_hbm, gain_hbm, tgt_hbm, temp_ref, tab_ref,
                pexp_ref, ptail_ref, peak_ref, stat_ref,
                win, twin, stg, mine, part, rx, tout, tin, stat_out, stat_in, stat_all, ubuf,
                hid_ref, gain_ref, tgt_ref,
                in_sem, win_sem, twin_sem, psend, precv, xsend, xrecv, tsend, trecv, srecv, go):
    me = lax.axis_index('tp')
    chip = me // 2
    core = me % 2
    partner = chip * 2 + (1 - core)
    across = (1 - chip) * 2 + core
    diag = (1 - chip) * 2 + (1 - core)
    shard = vocab // tp
    tokens, width = hid_hbm.shape
    chunk = NBLK * LANES
    nch = sum(GROUPS)
    steps = 2 * nch
    tail_at = nch * chunk
    last_blk = vocab // LANES - 1

    barrier = pltpu.get_barrier_semaphore()
    for peer in (partner, diag):
        pl.semaphore_signal(barrier, inc=1, device_id={'tp': peer}, device_id_type=MESH)

    @pl.when(core != FAR)
    def _():
        pl.semaphore_signal(barrier, inc=1, device_id={'tp': across}, device_id_type=MESH)

    small = [pltpu.make_async_copy(src, dst, in_sem.at[i % 2]) for i, (src, dst) in enumerate((
        (hid_hbm, hid_ref), (gain_hbm, gain_ref), (tgt_hbm, tgt_ref)))]

    def window(g, which):
        far = g < nch
        k = jnp.where(far, g, g - nch)
        there = jnp.where(far, 1 - chip, chip)
        dest = there * 2 + (jnp.where(which == 0, 1 - core, core))
        blk = (dest * shard) // LANES + k * NBLK
        slot = (g % DEPTH) * 2 + which
        return pltpu.make_async_copy(
            tab_ref.at[:, pl.ds(pl.multiple_of(blk * LANES, LANES), chunk + LANES)],
            win.at[slot], win_sem.at[slot]), dest, slot

    def fetch(g, which):
        window(g, which)[0].start()

    def tail_window(i, dest):
        blk = (dest * shard) // LANES + nch * NBLK
        edge = jnp.minimum(blk + TAIL, last_blk)
        for at, first, count in ((blk, 0, TAIL), (edge, TAIL, 1)):
            pltpu.make_async_copy(
                tab_ref.at[:, pl.ds(pl.multiple_of(at * LANES, LANES), count * LANES)],
                twin.at[i % 2, :, pl.ds(first * LANES, count * LANES)], twin_sem.at[i % 2]).start()

    tail_dests = ((1 - chip) * 2 + (1 - FAR), (1 - chip) * 2 + FAR, partner, me)
    small[0].start()
    small[1].start()
    fetch(0, 0)
    tail_window(0, tail_dests[0])
    tail_window(1, tail_dests[1])
    fetch(0, 1)
    small[0].wait()
    small[1].wait()

    x = hid_ref[...].astype(jnp.float32)
    inv_rms = lax.rsqrt(jnp.mean(x * x, axis=-1, keepdims=True) + NORM_EPS)
    gain = jnp.concatenate([gain_ref[i:i + 1] for i in range(width // LANES)], axis=1).astype(jnp.float32)
    own, own_gain = x[:, :rows], gain[:, :rows]
    for t in range(1, tp):
        cols = slice(t * rows, (t + 1) * rows)
        own = jnp.where(me == t, x[:, cols], own)
        own_gain = jnp.where(me == t, gain[:, cols], own_gain)
    ubuf[...] = (own * inv_rms * own_gain).astype(jnp.bfloat16)

    lane = lax.broadcasted_iota(jnp.int32, (tokens, LANES), 1)
    row = lax.broadcasted_iota(jnp.int32, (tokens, LANES), 0)

    def place(z, dest, blocks, store):
        back = LANES - (dest * shard) % LANES
        rolled = [pltpu.roll(z[:, b * LANES:(b + 1) * LANES], back, 1) for b in range(blocks + 1)]
        for b in range(blocks):
            store(b, jnp.where(lane < back, rolled[b], rolled[b + 1]))

    def tail_logits(i):
        pltpu.make_async_copy(tab_ref.at[:, pl.ds(0, (TAIL + 1) * LANES)], twin.at[i % 2], twin_sem.at[i % 2]).wait()

        def store(b, v):
            tout[i, :, b * LANES:(b + 1) * LANES] = v
        place(dot(ubuf[...], twin[i % 2]), tail_dests[i], TAIL, store)

    def tail_send(i):
        slot = 2 if i == 2 else (jnp.where(core == FAR, 1 - i, i))
        return pltpu.make_async_remote_copy(
            src_ref=tout.at[i], dst_ref=tin.at[slot], send_sem=tsend.at[0], recv_sem=trecv.at[0],
            device_id={'tp': tail_dests[i]}, device_id_type=MESH)

    def to_partner(g):
        return pltpu.make_async_remote_copy(
            src_ref=stg.at[g], dst_ref=part.at[g], send_sem=psend.at[0], recv_sem=precv.at[g % RING],
            device_id={'tp': partner}, device_id_type=MESH)

    starts = [sum(GROUPS[:i]) for i in range(len(GROUPS))]

    def owner(i):
        return sum(i >= end for end in JOINT[:-1])

    def to_across(i):
        chunks = pl.ds(starts[i], GROUPS[i])
        return pltpu.make_async_remote_copy(
            src_ref=mine.at[chunks], dst_ref=rx.at[chunks], send_sem=xsend.at[0], recv_sem=xrecv.at[owner(i)],
            device_id={'tp': across}, device_id_type=MESH)

    def partial_logits(g, which, out):
        copy, dest, slot = window(g, which)
        copy.wait()

        def store(b, v):
            out[g, :, b * LANES:(b + 1) * LANES] = v
        place(dot(ubuf[...], win[slot]), dest, NBLK, store)

    def combine(g):
        to_partner(g).wait_recv()
        mine[g] = mine[g] + part[g]

    def fetch_next(g, which):
        @pl.when(g + DEPTH < steps)
        def _():
            fetch(g + DEPTH, which)

    def hand_over(g):
        partial_logits(g, 0, stg)
        to_partner(g).start()
        fetch_next(g, 0)

    def keep(g):
        partial_logits(g, 1, mine)
        fetch_next(g, 1)

    partial_logits(0, 0, stg)
    fetch(1, 0)
    fetch(1, 1)
    fetch(2, 0)
    fetch(2, 1)
    small[2].start()
    tail_logits(0)

    @pl.when(core == FAR)
    def _():
        pl.semaphore_wait(barrier, 2)

    @pl.when(core != FAR)
    def _():
        pl.semaphore_wait(barrier, 3)
        pl.semaphore_signal(go, inc=1, device_id={'tp': partner}, device_id_type=MESH)

    to_partner(0).start()
    tail_send(0).start()
    tail_logits(1)

    @pl.when(core == FAR)
    def _():
        pl.semaphore_wait(go, 1)

    tail_send(1).start()
    fetch(DEPTH, 0)
    hand_over(1)
    keep(0)
    combine(0)
    to_across(0).start()
    hand_over(2)
    keep(1)
    combine(1)
    to_across(1).start()
    tail_window(2, partner)
    tail_window(3, me)

    def step(g, _):
        @pl.when(g + 1 < steps)
        def _():
            hand_over(g + 1)
        keep(g)
        h = g - 1

        @pl.when(h >= 2)
        def _():
            combine(h)

        for i, first in enumerate(starts[2:], 2):
            ready = first + GROUPS[i] - 1

            @pl.when(h == jnp.where(core == FAR, ready, ready if i < HELD else max(ready, HOLD)))
            def _():
                to_across(i).start()
        return 0

    lax.fori_loop(2, steps, step, 0)
    tail_logits(2)
    tail_send(2).start()
    tail_logits(3)
    combine(steps - 1)

    small[2].wait()
    factor = 1.0 / temp_ref[0]
    target = jnp.zeros((tokens, LANES), jnp.int32)
    for i in range(tokens):
        target = jnp.where(row == i, tgt_ref[i], target)
    target = target - me * shard
    target = jnp.where(target < shard, target, -1)

    def softmax_step(carry, at, ts, store):
        m, s, tg = carry
        new_m = m
        for b, t in enumerate(ts):
            tg = tg + jnp.where(lane + (at + b * LANES) == target, t, 0.0)
            new_m = jnp.maximum(new_m, t)
        s = s * jnp.exp(m - new_m)
        for b, t in enumerate(ts):
            p = jnp.exp(t - new_m)
            s = s + p
            store(b, p)
        return new_m, s, tg

    def absorb(k, carry):
        def store(b, p):
            pexp_ref[k, :, b * LANES:(b + 1) * LANES] = p
        ts = [(mine[nch + k, :, b * LANES:(b + 1) * LANES] + rx[k, :, b * LANES:(b + 1) * LANES]) * factor
              for b in range(NBLK)]
        carry = softmax_step(carry, k * chunk, ts, store)
        peak_ref[k] = carry[0]
        return carry

    def absorb_tail(carry):
        pltpu.make_async_copy(tin, tin, trecv.at[0]).wait()

        def store(b, p):
            ptail_ref[:, b * LANES:(b + 1) * LANES] = p
        ts = []
        for b in range(TAIL):
            cols = slice(b * LANES, (b + 1) * LANES)
            t = ((tout[3, :, cols] + tin[2, :, cols]) + (tin[0, :, cols] + tin[1, :, cols])) * factor
            ts.append(jnp.where(lane + (tail_at + b * LANES) < shard, t, -jnp.inf))
        carry = softmax_step(carry, tail_at, ts, store)
        peak_ref[nch] = carry[0]
        return carry

    def stat_send(i, peer):
        return pltpu.make_async_remote_copy(
            src_ref=stat_out, dst_ref=stat_in.at[i], send_sem=psend.at[0], recv_sem=srecv.at[i],
            device_id={'tp': peer}, device_id_type=MESH)

    def merge(a, b):
        big = jnp.maximum(a[0], b[0])
        return big, a[1] * jnp.exp(a[0] - big) + b[1] * jnp.exp(b[0] - big), a[2] + b[2]

    field = LANES // 8
    half = tokens // 2

    def received(i):
        stat_send(i, partner).wait_recv()
        columns = [stat_in[i, :, j * field:j * field + 1] for j in range(6)]
        wide = [jnp.broadcast_to(c, (half, LANES)) for c in columns]
        return [jnp.concatenate(wide[2 * j:2 * j + 2], axis=0) for j in range(3)]

    def put(values):
        tile = values[2][half:]
        fields = [v[lo:lo + half] for v in values for lo in (0, half)]
        for j in range(4, -1, -1):
            tile = jnp.where(lane[:half] < (j + 1) * field, fields[j], tile)
        stat_out[...] = tile

    def conclude(stats):
        big, total, picked = stats
        stat_ref[0] = big + jnp.log(total)
        stat_ref[1] = picked

    def take_partner(carry):
        big, total, picked = merge(carry, received(1))
        only = lane == 0
        alone = carry[1] * jnp.exp(carry[0] - big)
        return big, jnp.where(only, total, alone), jnp.where(only, picked, carry[2])

    pltpu.make_async_copy(stg, stg, psend.at[0]).wait()
    zeros = jnp.zeros((tokens, LANES), jnp.float32)
    carry = (zeros - jnp.inf, zeros, zeros)
    for j, end in enumerate(JOINT):
        begin = JOINT[j - 1] if j else 0
        if j == len(JOINT) - 1:
            carry = lax.cond(core == FAR, lambda c: c, take_partner, carry)
        first, count = starts[begin], sum(GROUPS[begin:end])
        arrived = rx.at[pl.ds(first, count)]
        pltpu.make_async_copy(arrived, arrived, xrecv.at[j]).wait()
        carry = absorb(first, carry) if count == 1 else lax.fori_loop(first, first + count, absorb, carry)
        if j == 0:
            carry = absorb_tail(carry)
    m, s, tg = carry

    top = jnp.max(m, axis=-1, keepdims=True)
    total = jnp.sum(s * jnp.exp(m - top), axis=-1, keepdims=True)
    picked = jnp.sum(tg, axis=-1, keepdims=True)
    own_stat = [jnp.broadcast_to(v, (tokens, LANES)) for v in (top, total, picked)]

    @pl.when(core == FAR)
    def _():
        put(own_stat)
        stat_send(1, partner).start()
        chip_stat = received(1)
        conclude(merge(chip_stat, received(0)))
        stat_send(1, partner).wait_send()

    @pl.when(core != FAR)
    def _():
        chip_stat = own_stat
        put(chip_stat)
        stat_send(0, diag).start()
        stat_send(0, across).start()
        stat_send(1, partner).start()
        conclude(merge(chip_stat, received(0)))
        pltpu.make_async_copy(stat_all, stat_all, psend.at[0]).wait()

    pltpu.make_async_copy(rx, rx, xsend.at[0]).wait()
    pltpu.make_async_copy(tin, tin, tsend.at[0]).wait()


def finish_kernel(pexp_ref, ptail_ref, peak_ref, stat_ref, probs_hbm, ln_hbm, tl_hbm,
                  buf, ln_buf, tl_buf, sem, vec_sem):
    tokens = stat_ref.shape[1]
    nch, _, chunk = pexp_ref.shape
    shard = buf.shape[1]
    log_norm = stat_ref[0]
    picked = stat_ref[1]
    copies = []
    for j in range(len(PIECES) - 1):
        lo, hi = PIECES[j], PIECES[j + 1]
        for k in range(lo, hi):
            scale = jnp.exp(peak_ref[k] - log_norm)
            for b in range(chunk // LANES):
                p = pexp_ref[k, :, b * LANES:(b + 1) * LANES] * scale
                buf[:, k * chunk + b * LANES:k * chunk + (b + 1) * LANES] = p.astype(jnp.bfloat16)
        end = hi * chunk
        if j == len(PIECES) - 2:
            scale = jnp.exp(peak_ref[nch] - log_norm)
            for at in range(end, shard, LANES):
                p = (ptail_ref[:, at - end:at - end + LANES] * scale).astype(jnp.bfloat16)
                buf[:, at:min(at + LANES, shard)] = p[:, :min(LANES, shard - at)]
            end = shard
        cols = pl.ds(lo * chunk, end - lo * chunk)
        copies.append(pltpu.make_async_copy(buf.at[:, cols], probs_hbm.at[:, cols], sem.at[j]))
        copies[-1].start()
        if j == 3:
            lane = lax.broadcasted_iota(jnp.int32, (tokens, LANES), 1)
            row = lax.broadcasted_iota(jnp.int32, (tokens, LANES), 0)
            for i, (tmp, out, val) in enumerate(((ln_buf, ln_hbm, log_norm),
                                                 (tl_buf, tl_hbm, picked - log_norm))):
                tmp[...] = jnp.sum(jnp.where(row == lane, val, 0.0), axis=0)[:tokens]
                copies.append(pltpu.make_async_copy(tmp, out, vec_sem.at[i]))
                copies[-1].start()
    for copy in copies:
        copy.wait()


def solution(mesh):
    tp = mesh.shape['tp']

    def local_scores(hidden, final_gain, table_cols, targets, temperature):
        tokens, width = hidden.shape
        vocab, rows = table_cols.shape
        shard = vocab // tp
        chunk = NBLK * LANES
        nch = sum(GROUPS)
        f32, bf16 = jnp.float32, jnp.bfloat16

        def body(*refs):
            head_kernel(rows, vocab, tp, *refs)

        def in_hbm(a):
            return pltpu.with_memory_space_constraint(a, pltpu.HBM)

        def dma(n):
            return pltpu.SemaphoreType.DMA((n,))

        vm = pl.BlockSpec(memory_space=pltpu.VMEM)
        hbm = pl.BlockSpec(memory_space=pltpu.HBM)
        outs = pl.pallas_call(
            body,
            out_shape=(pltpu.VMEM((nch, tokens, chunk), f32),
                       pltpu.VMEM((tokens, TAIL * LANES), f32),
                       pltpu.VMEM((nch + 1, tokens, LANES), f32),
                       pltpu.VMEM((2, tokens, LANES), f32)),
            in_specs=[hbm, hbm, hbm, pl.BlockSpec(memory_space=pltpu.SMEM), hbm],
            out_specs=(vm, vm, vm, vm),
            scratch_shapes=[
                pltpu.VMEM((DEPTH * 2, rows, chunk + LANES), bf16),
                pltpu.VMEM((2, rows, (TAIL + 1) * LANES), bf16),
                pltpu.VMEM((2 * nch, tokens, chunk), f32),
                pltpu.VMEM((2 * nch, tokens, chunk), f32),
                pltpu.VMEM((2 * nch, tokens, chunk), f32),
                pltpu.VMEM((nch, tokens, chunk), f32),
                pltpu.VMEM((4, tokens, TAIL * LANES), f32),
                pltpu.VMEM((3, tokens, TAIL * LANES), f32),
                pltpu.VMEM((tokens // 2, LANES), f32),
                pltpu.VMEM((2, tokens // 2, LANES), f32),
                pltpu.VMEM((3, tokens // 2, LANES), f32),
                pltpu.VMEM((tokens, rows), bf16),
                pltpu.VMEM((tokens, width), bf16),
                pltpu.VMEM((width // LANES, LANES), bf16),
                pltpu.SMEM((tokens,), jnp.int32),
                dma(2), dma(DEPTH * 2), dma(2), dma(1), dma(RING), dma(1), dma(len(JOINT)),
                dma(1), dma(1), dma(2), pltpu.SemaphoreType.REGULAR,
            ],
            compiler_params=pltpu.CompilerParams(
                collective_id=0, has_side_effects=True, vmem_limit_bytes=40 * 1024 * 1024),
        )(in_hbm(hidden), in_hbm(final_gain.reshape(width // LANES, LANES)), in_hbm(targets),
          temperature.reshape(1), in_hbm(table_cols.T))
        probs, ln, tl = pl.pallas_call(
            finish_kernel,
            out_shape=(pltpu.HBM((tokens, shard), bf16), pltpu.HBM((tokens,), f32), pltpu.HBM((tokens,), f32)),
            in_specs=[vm, vm, vm, vm],
            out_specs=(hbm, hbm, hbm),
            scratch_shapes=[
                pltpu.VMEM((tokens, shard), bf16), pltpu.VMEM((tokens,), f32), pltpu.VMEM((tokens,), f32),
                dma(len(PIECES) - 1), dma(2),
            ],
            compiler_params=pltpu.CompilerParams(vmem_limit_bytes=8 * 1024 * 1024),
        )(*(pltpu.with_memory_space_constraint(a, pltpu.VMEM) for a in outs))
        return ln, tl, probs

    return jax.shard_map(local_scores, mesh=mesh,
                         in_specs=(P('dp', None), P(None), P(None, 'tp'), P('dp'), P()),
                         out_specs=(P('dp'), P('dp'), P('dp', 'tp')),
                         check_vma=False)
```

```python
import jax
import jax.numpy as jnp
from jax import lax
from jax.experimental import pallas as pl
from jax.experimental.pallas import tpu as pltpu
from jax.sharding import PartitionSpec as P

NORM_EPS = 1e-6
LANES = 128
NBLK = 7
TAIL = 3
DEPTH = 3
RING = 6
GROUPS = (1, 1, 2, 4, 6, 8, 8, 11, 1)
FAR = 0
HELD = 5
HOLD = 36
JOINT = (7, 8, 9)
PIECES = (0, 2, 12, 22, 32, 42)
MESH = pl.DeviceIdType.MESH


def dot(u, window):
    return jnp.dot(u, window, preferred_element_type=jnp.float32)


def head_kernel(rows, vocab, tp,
                hid_hbm, gain_hbm, tgt_hbm, temp_ref, tab_ref,
                pexp_ref, ptail_ref, peak_ref, stat_ref,
                win, twin, stg, mine, part, rx, tout, tin, stat_out, stat_in, stat_all, ubuf,
                hid_ref, gain_ref, tgt_ref,
                in_sem, win_sem, twin_sem, psend, precv, xsend, xrecv, tsend, trecv, srecv, go):
    me = lax.axis_index('tp')
    chip = me // 2
    core = me % 2
    partner = chip * 2 + (1 - core)
    across = (1 - chip) * 2 + core
    diag = (1 - chip) * 2 + (1 - core)
    shard = vocab // tp
    tokens, width = hid_hbm.shape
    chunk = NBLK * LANES
    nch = sum(GROUPS)
    steps = 2 * nch
    tail_at = nch * chunk
    last_blk = vocab // LANES - 1

    barrier = pltpu.get_barrier_semaphore()
    @pl.when(core != FAR)
    def _():
        pl.semaphore_signal(barrier, inc=1, device_id={'tp': across}, device_id_type=MESH)

    for peer in (diag, partner):
        pl.semaphore_signal(barrier, inc=1, device_id={'tp': peer}, device_id_type=MESH)

    small = [pltpu.make_async_copy(src, dst, in_sem.at[i % 2]) for i, (src, dst) in enumerate((
        (hid_hbm, hid_ref), (gain_hbm, gain_ref), (tgt_hbm, tgt_ref)))]

    def window(g, which):
        far = g < nch
        k = jnp.where(far, g, g - nch)
        there = jnp.where(far, 1 - chip, chip)
        dest = there * 2 + (jnp.where(which == 0, 1 - core, core))
        blk = (dest * shard) // LANES + k * NBLK
        slot = (g % DEPTH) * 2 + which
        return pltpu.make_async_copy(
            tab_ref.at[:, pl.ds(pl.multiple_of(blk * LANES, LANES), chunk + LANES)],
            win.at[slot], win_sem.at[slot]), dest, slot

    def fetch(g, which):
        window(g, which)[0].start()

    def tail_window(i, dest):
        blk = (dest * shard) // LANES + nch * NBLK
        edge = jnp.minimum(blk + TAIL, last_blk)
        for at, first, count in ((blk, 0, TAIL), (edge, TAIL, 1)):
            pltpu.make_async_copy(
                tab_ref.at[:, pl.ds(pl.multiple_of(at * LANES, LANES), count * LANES)],
                twin.at[i % 2, :, pl.ds(first * LANES, count * LANES)], twin_sem.at[i % 2]).start()

    tail_dests = ((1 - chip) * 2 + (1 - FAR), (1 - chip) * 2 + FAR, partner, me)
    small[0].start()
    small[1].start()
    fetch(0, 0)
    tail_window(0, tail_dests[0])
    tail_window(1, tail_dests[1])
    fetch(0, 1)
    small[0].wait()
    small[1].wait()

    x = hid_ref[...].astype(jnp.float32)
    inv_rms = lax.rsqrt(jnp.mean(x * x, axis=-1, keepdims=True) + NORM_EPS)
    gain = jnp.concatenate([gain_ref[i:i + 1] for i in range(width // LANES)], axis=1).astype(jnp.float32)
    own, own_gain = x[:, :rows], gain[:, :rows]
    for t in range(1, tp):
        cols = slice(t * rows, (t + 1) * rows)
        own = jnp.where(me == t, x[:, cols], own)
        own_gain = jnp.where(me == t, gain[:, cols], own_gain)
    ubuf[...] = (own * inv_rms * own_gain).astype(jnp.bfloat16)

    lane = lax.broadcasted_iota(jnp.int32, (tokens, LANES), 1)
    row = lax.broadcasted_iota(jnp.int32, (tokens, LANES), 0)

    def place(z, dest, blocks, store):
        back = LANES - (dest * shard) % LANES
        rolled = [pltpu.roll(z[:, b * LANES:(b + 1) * LANES], back, 1) for b in range(blocks + 1)]
        for b in range(blocks):
            store(b, jnp.where(lane < back, rolled[b], rolled[b + 1]))

    def tail_logits(i):
        pltpu.make_async_copy(tab_ref.at[:, pl.ds(0, (TAIL + 1) * LANES)], twin.at[i % 2], twin_sem.at[i % 2]).wait()

        def store(b, v):
            tout[i, :, b * LANES:(b + 1) * LANES] = v
        place(dot(ubuf[...], twin[i % 2]), tail_dests[i], TAIL, store)

    def tail_send(i):
        slot = 2 if i == 2 else (jnp.where(core == FAR, 1 - i, i))
        return pltpu.make_async_remote_copy(
            src_ref=tout.at[i], dst_ref=tin.at[slot], send_sem=tsend.at[0], recv_sem=trecv.at[0],
            device_id={'tp': tail_dests[i]}, device_id_type=MESH)

    def to_partner(g):
        return pltpu.make_async_remote_copy(
            src_ref=stg.at[g], dst_ref=part.at[g], send_sem=psend.at[0], recv_sem=precv.at[g % RING],
            device_id={'tp': partner}, device_id_type=MESH)

    starts = [sum(GROUPS[:i]) for i in range(len(GROUPS))]

    def owner(i):
        return sum(i >= end for end in JOINT[:-1])

    def to_across(i):
        chunks = pl.ds(starts[i], GROUPS[i])
        return pltpu.make_async_remote_copy(
            src_ref=mine.at[chunks], dst_ref=rx.at[chunks], send_sem=xsend.at[0], recv_sem=xrecv.at[owner(i)],
            device_id={'tp': across}, device_id_type=MESH)

    def partial_logits(g, which, out):
        copy, dest, slot = window(g, which)
        copy.wait()

        def store(b, v):
            out[g, :, b * LANES:(b + 1) * LANES] = v
        place(dot(ubuf[...], win[slot]), dest, NBLK, store)

    def combine(g):
        to_partner(g).wait_recv()
        mine[g] = mine[g] + part[g]

    def fetch_next(g, which):
        @pl.when(g + DEPTH < steps)
        def _():
            fetch(g + DEPTH, which)

    def hand_over(g):
        partial_logits(g, 0, stg)
        to_partner(g).start()
        fetch_next(g, 0)

    def keep(g):
        partial_logits(g, 1, mine)
        fetch_next(g, 1)

    partial_logits(0, 0, stg)
    fetch(1, 0)
    fetch(1, 1)
    fetch(2, 0)
    fetch(2, 1)
    small[2].start()
    tail_logits(0)

    @pl.when(core == FAR)
    def _():
        pl.semaphore_wait(barrier, 2)

    @pl.when(core != FAR)
    def _():
        pl.semaphore_wait(barrier, 3)
        pl.semaphore_signal(go, inc=1, device_id={'tp': partner}, device_id_type=MESH)

    to_partner(0).start()
    tail_send(0).start()
    tail_logits(1)

    @pl.when(core == FAR)
    def _():
        pl.semaphore_wait(go, 1)

    tail_send(1).start()
    fetch(DEPTH, 0)
    hand_over(1)
    keep(0)
    combine(0)
    to_across(0).start()
    hand_over(2)
    keep(1)
    combine(1)
    to_across(1).start()
    tail_window(2, partner)
    tail_window(3, me)

    def step(g, _):
        @pl.when(g + 1 < steps)
        def _():
            hand_over(g + 1)
        keep(g)
        h = g - 1

        @pl.when(h >= 2)
        def _():
            combine(h)

        for i, first in enumerate(starts[2:], 2):
            ready = first + GROUPS[i] - 1

            @pl.when(h == jnp.where(core == FAR, ready, ready if i < HELD else max(ready, HOLD)))
            def _():
                to_across(i).start()
        return 0

    lax.fori_loop(2, steps, step, 0)
    tail_logits(2)
    tail_send(2).start()
    tail_logits(3)
    combine(steps - 1)

    small[2].wait()
    factor = 1.0 / temp_ref[0]
    target = jnp.zeros((tokens, LANES), jnp.int32)
    for i in range(tokens):
        target = jnp.where(row == i, tgt_ref[i], target)
    target = target - me * shard
    target = jnp.where(target < shard, target, -1)

    def softmax_step(carry, at, ts, store):
        m, s, tg = carry
        new_m = m
        for b, t in enumerate(ts):
            tg = tg + jnp.where(lane + (at + b * LANES) == target, t, 0.0)
            new_m = jnp.maximum(new_m, t)
        s = s * jnp.exp(m - new_m)
        for b, t in enumerate(ts):
            p = jnp.exp(t - new_m)
            s = s + p
            store(b, p)
        return new_m, s, tg

    def absorb(k, carry):
        def store(b, p):
            pexp_ref[k, :, b * LANES:(b + 1) * LANES] = p
        ts = [(mine[nch + k, :, b * LANES:(b + 1) * LANES] + rx[k, :, b * LANES:(b + 1) * LANES]) * factor
              for b in range(NBLK)]
        carry = softmax_step(carry, k * chunk, ts, store)
        peak_ref[k] = carry[0]
        return carry

    def absorb_tail(carry):
        pltpu.make_async_copy(tin, tin, trecv.at[0]).wait()

        def store(b, p):
            ptail_ref[:, b * LANES:(b + 1) * LANES] = p
        ts = []
        for b in range(TAIL):
            cols = slice(b * LANES, (b + 1) * LANES)
            t = ((tout[3, :, cols] + tin[2, :, cols]) + (tin[0, :, cols] + tin[1, :, cols])) * factor
            ts.append(jnp.where(lane + (tail_at + b * LANES) < shard, t, -jnp.inf))
        carry = softmax_step(carry, tail_at, ts, store)
        peak_ref[nch] = carry[0]
        return carry

    def stat_send(i, peer):
        return pltpu.make_async_remote_copy(
            src_ref=stat_out, dst_ref=stat_in.at[i], send_sem=psend.at[0], recv_sem=precv.at[0] if i else srecv.at[0],
            device_id={'tp': peer}, device_id_type=MESH)

    def merge(a, b):
        big = jnp.maximum(a[0], b[0])
        return big, a[1] * jnp.exp(a[0] - big) + b[1] * jnp.exp(b[0] - big), a[2] + b[2]

    field = LANES // 8
    half = tokens // 2

    def received(i):
        stat_send(i, partner).wait_recv()
        columns = [stat_in[i, :, j * field:j * field + 1] for j in range(6)]
        wide = [jnp.broadcast_to(c, (half, LANES)) for c in columns]
        return [jnp.concatenate(wide[2 * j:2 * j + 2], axis=0) for j in range(3)]

    def put(values):
        tile = values[2][half:]
        fields = [v[lo:lo + half] for v in values for lo in (0, half)]
        for j in range(4, -1, -1):
            tile = jnp.where(lane[:half] < (j + 1) * field, fields[j], tile)
        stat_out[...] = tile

    def conclude(stats):
        big, total, picked = stats
        stat_ref[0] = big + jnp.log(total)
        stat_ref[1] = picked

    def take_partner(carry):
        big, total, picked = merge(carry, received(1))
        only = lane == 0
        alone = carry[1] * jnp.exp(carry[0] - big)
        return big, jnp.where(only, total, alone), jnp.where(only, picked, carry[2])

    pltpu.make_async_copy(stg, stg, psend.at[0]).wait()
    zeros = jnp.zeros((tokens, LANES), jnp.float32)
    carry = (zeros - jnp.inf, zeros, zeros)
    for j, end in enumerate(JOINT):
        begin = JOINT[j - 1] if j else 0
        if j == len(JOINT) - 1:
            carry = lax.cond(core == FAR, lambda c: c, take_partner, carry)
        first, count = starts[begin], sum(GROUPS[begin:end])
        arrived = rx.at[pl.ds(first, count)]
        pltpu.make_async_copy(arrived, arrived, xrecv.at[j]).wait()
        carry = absorb(first, carry) if count == 1 else lax.fori_loop(first, first + count, absorb, carry)
        if j == 0:
            carry = absorb_tail(carry)
    m, s, tg = carry

    top = jnp.max(m, axis=-1, keepdims=True)
    total = jnp.sum(s * jnp.exp(m - top), axis=-1, keepdims=True)
    picked = jnp.sum(tg, axis=-1, keepdims=True)
    own_stat = [jnp.broadcast_to(v, (tokens, LANES)) for v in (top, total, picked)]

    @pl.when(core == FAR)
    def _():
        put(own_stat)
        stat_send(1, partner).start()
        chip_stat = received(1)
        conclude(merge(chip_stat, received(0)))
        stat_send(1, partner).wait_send()

    @pl.when(core != FAR)
    def _():
        chip_stat = own_stat
        put(chip_stat)
        stat_send(0, diag).start()
        stat_send(0, across).start()
        stat_send(1, partner).start()
        conclude(merge(chip_stat, received(0)))
        pltpu.make_async_copy(stat_all, stat_all, psend.at[0]).wait()

    pltpu.make_async_copy(rx, rx, xsend.at[0]).wait()
    pltpu.make_async_copy(tin, tin, tsend.at[0]).wait()


def finish_kernel(pexp_ref, ptail_ref, peak_ref, stat_ref, probs_hbm, ln_hbm, tl_hbm,
                  buf, ln_buf, tl_buf, sem, vec_sem):
    tokens = stat_ref.shape[1]
    nch, _, chunk = pexp_ref.shape
    shard = buf.shape[1]
    log_norm = stat_ref[0]
    picked = stat_ref[1]
    copies = []
    for j in range(len(PIECES) - 1):
        lo, hi = PIECES[j], PIECES[j + 1]
        for k in range(lo, hi):
            scale = jnp.exp(peak_ref[k] - log_norm)
            for b in range(chunk // LANES):
                p = pexp_ref[k, :, b * LANES:(b + 1) * LANES] * scale
                buf[:, k * chunk + b * LANES:k * chunk + (b + 1) * LANES] = p.astype(jnp.bfloat16)
        end = hi * chunk
        if j == len(PIECES) - 2:
            scale = jnp.exp(peak_ref[nch] - log_norm)
            for at in range(end, shard, LANES):
                p = (ptail_ref[:, at - end:at - end + LANES] * scale).astype(jnp.bfloat16)
                buf[:, at:min(at + LANES, shard)] = p[:, :min(LANES, shard - at)]
            end = shard
        cols = pl.ds(lo * chunk, end - lo * chunk)
        copies.append(pltpu.make_async_copy(buf.at[:, cols], probs_hbm.at[:, cols], sem.at[j]))
        copies[-1].start()
        if j == 3:
            lane = lax.broadcasted_iota(jnp.int32, (tokens, LANES), 1)
            row = lax.broadcasted_iota(jnp.int32, (tokens, LANES), 0)
            for i, (tmp, out, val) in enumerate(((ln_buf, ln_hbm, log_norm),
                                                 (tl_buf, tl_hbm, picked - log_norm))):
                tmp[...] = jnp.sum(jnp.where(row == lane, val, 0.0), axis=0)[:tokens]
                copies.append(pltpu.make_async_copy(tmp, out, vec_sem.at[i]))
                copies[-1].start()
    for copy in copies:
        copy.wait()


def solution(mesh):
    tp = mesh.shape['tp']

    def local_scores(hidden, final_gain, table_cols, targets, temperature):
        tokens, width = hidden.shape
        vocab, rows = table_cols.shape
        shard = vocab // tp
        chunk = NBLK * LANES
        nch = sum(GROUPS)
        f32, bf16 = jnp.float32, jnp.bfloat16

        def body(*refs):
            head_kernel(rows, vocab, tp, *refs)

        def in_hbm(a):
            return pltpu.with_memory_space_constraint(a, pltpu.HBM)

        def dma(n):
            return pltpu.SemaphoreType.DMA((n,))

        vm = pl.BlockSpec(memory_space=pltpu.VMEM)
        hbm = pl.BlockSpec(memory_space=pltpu.HBM)
        outs = pl.pallas_call(
            body,
            out_shape=(pltpu.VMEM((nch, tokens, chunk), f32),
                       pltpu.VMEM((tokens, TAIL * LANES), f32),
                       pltpu.VMEM((nch + 1, tokens, LANES), f32),
                       pltpu.VMEM((2, tokens, LANES), f32)),
            in_specs=[hbm, hbm, hbm, pl.BlockSpec(memory_space=pltpu.SMEM), hbm],
            out_specs=(vm, vm, vm, vm),
            scratch_shapes=[
                pltpu.VMEM((DEPTH * 2, rows, chunk + LANES), bf16),
                pltpu.VMEM((2, rows, (TAIL + 1) * LANES), bf16),
                pltpu.VMEM((2 * nch, tokens, chunk), f32),
                pltpu.VMEM((2 * nch, tokens, chunk), f32),
                pltpu.VMEM((2 * nch, tokens, chunk), f32),
                pltpu.VMEM((nch, tokens, chunk), f32),
                pltpu.VMEM((4, tokens, TAIL * LANES), f32),
                pltpu.VMEM((3, tokens, TAIL * LANES), f32),
                pltpu.VMEM((tokens // 2, LANES), f32),
                pltpu.VMEM((2, tokens // 2, LANES), f32),
                pltpu.VMEM((3, tokens // 2, LANES), f32),
                pltpu.VMEM((tokens, rows), bf16),
                pltpu.VMEM((tokens, width), bf16),
                pltpu.VMEM((width // LANES, LANES), bf16),
                pltpu.SMEM((tokens,), jnp.int32),
                dma(2), dma(DEPTH * 2), dma(2), dma(1), dma(RING), dma(1), dma(len(JOINT)),
                dma(1), dma(1), dma(1), pltpu.SemaphoreType.REGULAR,
            ],
            compiler_params=pltpu.CompilerParams(
                collective_id=0, has_side_effects=True, vmem_limit_bytes=40 * 1024 * 1024),
        )(in_hbm(hidden), in_hbm(final_gain.reshape(width // LANES, LANES)), in_hbm(targets),
          temperature.reshape(1), in_hbm(table_cols.T))
        probs, ln, tl = pl.pallas_call(
            finish_kernel,
            out_shape=(pltpu.HBM((tokens, shard), bf16), pltpu.HBM((tokens,), f32), pltpu.HBM((tokens,), f32)),
            in_specs=[vm, vm, vm, vm],
            out_specs=(hbm, hbm, hbm),
            scratch_shapes=[
                pltpu.VMEM((tokens, shard), bf16), pltpu.VMEM((tokens,), f32), pltpu.VMEM((tokens,), f32),
                dma(len(PIECES) - 1), dma(2),
            ],
            compiler_params=pltpu.CompilerParams(vmem_limit_bytes=8 * 1024 * 1024),
        )(*(pltpu.with_memory_space_constraint(a, pltpu.VMEM) for a in outs))
        return ln, tl, probs

    return jax.shard_map(local_scores, mesh=mesh,
                         in_specs=(P('dp', None), P(None), P(None, 'tp'), P('dp'), P()),
                         out_specs=(P('dp'), P('dp'), P('dp', 'tp')),
                         check_vma=False)
```
